16 devices in a mesh: dp: 4 (over z, y), ep: 4 (over x, core).
Axes of the slice: x: 2, y: 2, z: 2, core: 2. Of those that a mesh axis runs over, the one named last changes fastest.
Arguments:
- x_rows: bfloat16 [4096, 2048], P(('dp', 'ep')), parts along dimension 0
- logits: float32 [4096, 64], P(('dp', 'ep')), parts along dimension 0
- w_in: bfloat16 [64, 2048, 1408], P('ep')
- w_out: bfloat16 [64, 1408, 2048], P('ep')
Outputs:
- output: bfloat16 [4096, 2048], P(('dp', 'ep')), parts along dimension 0
There are 4 independent parts. The reference program is written for one: setup_inputs(seed, part) draws one part's arguments, and reference() takes and returns one part's arrays. A program takes and returns all parts, laid end to end along the dimension named above; an argument that names none is the same for every part.
All inputs are finite; a program needn't handle non-finite values.
Results may differ from the reference program's by a relative error of at most 0.001.
Values are sent between devices in bfloat16 or wider.
A program may use at most 1 GiB of HBM per device.

```python
import math
import jax
import jax.numpy as jnp
from jax import lax

TOKENS = 1024
D_MODEL = 2048
FF_HIDDEN = 1408
EXPERTS = 64
CAPACITY = 32
GROUP_DEV = 4
LOGIT_SHIFT = int(1024 * math.log(EXPERTS))


def draw_logits(route_key):
    sub_keys = jax.random.split(route_key, 5)
    tok_dev = TOKENS // GROUP_DEV
    mean_cnt = 2 * tok_dev // EXPERTS
    quarter = EXPERTS // 4
    exp_order = jax.random.permutation(sub_keys[0], EXPERTS)
    rot_bits = jax.random.randint(sub_keys[1], (GROUP_DEV,), 0, 2)
    tier_vals = jnp.array([2 * mean_cnt, mean_cnt, mean_cnt // 2, mean_cnt // 2], dtype=jnp.int32)
    tier_idx = (jnp.arange(EXPERTS)[None, :] // quarter + rot_bits[:, None]) % 4
    slot_ends = jnp.cumsum(tier_vals[tier_idx], axis=1)
    slot_ids = jnp.arange(2 * tok_dev)
    rank_pos = jnp.sum((slot_ends[:, None, :] <= slot_ids[None, :, None]).astype(jnp.int32), axis=2)
    pick_list = exp_order[rank_pos]
    perm_keys = jax.random.split(sub_keys[2], GROUP_DEV)
    tok_perm = jax.vmap(lambda perm_key: jax.random.permutation(perm_key, tok_dev))(perm_keys)
    first_pick = jnp.take_along_axis(pick_list[:, :tok_dev], tok_perm, axis=1).reshape(TOKENS)
    second_pick = jnp.take_along_axis(pick_list[:, tok_dev:], tok_perm, axis=1).reshape(TOKENS)
    expert_ids = jnp.arange(EXPERTS)
    chosen = (expert_ids[None, :] == first_pick[:, None]) | (expert_ids[None, :] == second_pick[:, None])
    base_val = jax.random.randint(sub_keys[3], (TOKENS, EXPERTS), 0, 2048)
    pick_val = jax.random.randint(sub_keys[4], (TOKENS, EXPERTS), 1024, 3072) + LOGIT_SHIFT
    score_int = jnp.where(chosen, pick_val, base_val) * EXPERTS + expert_ids[None, :]
    return score_int.astype(jnp.float32) / (1024.0 * EXPERTS)


def setup_inputs(seed: int = 0, part: int = 0) -> dict:
    part_key = jax.random.fold_in(jax.random.key(seed), part)
    sub_keys = jax.random.split(part_key, 2)
    w_keys = jax.random.split(jax.random.key(seed + 1), 2)
    x_rows = jax.random.normal(sub_keys[0], (TOKENS, D_MODEL), jnp.float32).astype(jnp.bfloat16)
    logits = draw_logits(sub_keys[1])
    w_in = (jax.random.normal(w_keys[0], (EXPERTS, D_MODEL, FF_HIDDEN), jnp.float32) * D_MODEL ** -0.5).astype(jnp.bfloat16)
    w_out = (jax.random.normal(w_keys[1], (EXPERTS, FF_HIDDEN, D_MODEL), jnp.float32) * (2.0 * FF_HIDDEN ** -0.5)).astype(jnp.bfloat16)
    return {'x_rows': x_rows, 'logits': logits, 'w_in': w_in, 'w_out': w_out}


def reference(x_rows, logits, w_in, w_out):
    gate_probs = jax.nn.softmax(logits, axis=-1)
    top_vals, top_ids = lax.top_k(logits, 2)
    chosen = (logits >= top_vals[:, 1:2]).astype(jnp.int32)
    before = jnp.cumsum(chosen, axis=0) - chosen
    pick_pos = jnp.take_along_axis(before, top_ids, axis=1)
    dest_row = jnp.where(pick_pos < CAPACITY, top_ids * CAPACITY + pick_pos, EXPERTS * CAPACITY)
    tok_ids = jnp.broadcast_to(jnp.arange(TOKENS, dtype=jnp.int32)[:, None], (TOKENS, 2))
    slot_tok = jnp.full((EXPERTS * CAPACITY,), TOKENS, jnp.int32).at[dest_row.reshape(-1)].set(tok_ids.reshape(-1), mode='drop')
    expert_rows = jnp.take(x_rows, slot_tok, axis=0, mode='fill', fill_value=0).reshape(EXPERTS, CAPACITY, D_MODEL)

    def expert_ffn(operands):
        rows_in, w_first, w_second = operands
        hidden = jax.nn.gelu(jnp.dot(rows_in, w_first, preferred_element_type=jnp.float32), approximate=True).astype(jnp.bfloat16)
        return jnp.dot(hidden, w_second, preferred_element_type=jnp.float32).astype(jnp.bfloat16)

    expert_out = lax.map(expert_ffn, (expert_rows, w_in, w_out)).reshape(EXPERTS * CAPACITY, D_MODEL)
    rows_back = jnp.take(expert_out, dest_row, axis=0, mode='fill', fill_value=0)
    pick_gate = jnp.take_along_axis(gate_probs, top_ids, axis=1)
    mix_sum = jnp.sum(pick_gate[:, :, None] * rows_back.astype(jnp.float32), axis=1)
    return (x_rows.astype(jnp.float32) + mix_sum).astype(jnp.bfloat16)
```

```python
import functools

import jax
import jax.numpy as jnp
from jax import lax
from jax.experimental import pallas as pl
from jax.experimental.pallas import tpu as pltpu
from jax.sharding import PartitionSpec as P

BF16 = jnp.bfloat16
F32 = jnp.float32
MESH = pl.DeviceIdType.MESH
NREL = 4
NCH = 4
NS1 = 12
NS2 = 3
PAIR = 2


def iota(shape, dim):
    return lax.broadcasted_iota(jnp.int32, shape, dim)


def moe_kernel(cap, x_hbm, logits_ref, w1_hbm, w2_hbm, out_ref, xall, st_own, st_all, dmat, xg, hacc, hb, w1buf, w2buf,
               zs, zr, acc, w1_sem, w2_sem, xl_sem, xs_sem, xr_sem, ss_sem, sr_sem, zs_sem, zr_sem):
    tok, nexp = logits_ref.shape
    edev, d_model, ff = w1_hbm.shape
    src_cap = xg.shape[2]
    slots = edev * src_cap
    ck = d_model // NCH
    rows = NREL * src_cap
    eblk = zr.shape[1] // rows
    nblk = edev // eblk

    me = lax.axis_index('ep')
    mx, mc = me // 2, me % 2
    dev = [me, 2 * mx + (1 - mc), 2 * (1 - mx) + mc, 2 * (1 - mx) + (1 - mc)]

    def w1_copy(i):
        c, e = i // edev, i % edev
        k = pl.multiple_of(c * ck, ck)
        s = i % NS1
        return pltpu.make_async_copy(w1_hbm.at[e, pl.ds(k, ck), :], w1buf.at[s], w1_sem.at[s])

    def w2_copy(e):
        s = e % NS2
        return pltpu.make_async_copy(w2_hbm.at[e], w2buf.at[s], w2_sem.at[s])

    def x_local(c):
        return pltpu.make_async_copy(x_hbm.at[:, pl.ds(c * ck, ck)], xall.at[0, c], xl_sem.at[c])

    def x_remote(c, slot):
        src = xall.at[2 if slot == 3 else 0, c]
        return pltpu.make_async_remote_copy(src_ref=src, dst_ref=xall.at[slot, c], send_sem=xs_sem.at[slot - 1, c],
                                            recv_sem=xr_sem.at[slot - 1, c],
                                            device_id={'ep': dev[2 if slot == 2 else 1]}, device_id_type=MESH)

    def s_remote(r):
        first = pl.multiple_of(dev[r] * edev, edev)
        return pltpu.make_async_remote_copy(src_ref=st_own.at[pl.ds(first, edev), :], dst_ref=st_all.at[r],
                                            send_sem=ss_sem.at[r - 1], recv_sem=sr_sem.at[r - 1],
                                            device_id={'ep': dev[r]}, device_id_type=MESH)

    def z_remote(e, r):
        b, q = e // eblk, e % eblk
        first = pl.multiple_of(r * (eblk * src_cap) + q * src_cap, src_cap)
        return pltpu.make_async_remote_copy(src_ref=zs.at[e, pl.ds(r * src_cap, src_cap), :],
                                            dst_ref=zr.at[b, pl.ds(first, src_cap), :],
                                            send_sem=zs_sem.at[r - 1, b], recv_sem=zr_sem.at[r - 1, b],
                                            device_id={'ep': dev[r]}, device_id_type=MESH)

    def z_block(b, r):
        part = zr.at[b, pl.ds(r * eblk * src_cap, eblk * src_cap), :]
        return pltpu.make_async_remote_copy(src_ref=part, dst_ref=part, send_sem=zs_sem.at[r - 1, b],
                                            recv_sem=zr_sem.at[r - 1, b], device_id={'ep': dev[r]}, device_id_type=MESH)

    barrier = pltpu.get_barrier_semaphore()
    for r in range(1, NREL):
        pl.semaphore_signal(barrier, inc=1, device_id={'ep': dev[r]}, device_id_type=MESH)
    for c in range(NCH):
        x_local(c).start()

    def start_w1(i, carry):
        w1_copy(i).start()
        return carry
    lax.fori_loop(0, NS1, start_w1, 0)
    for e in range(NS2):
        w2_copy(e).start()

    pl.semaphore_wait(barrier, NREL - 1)
    x_local(0).wait()
    x_remote(0, 2).start()
    x_remote(0, 1).start()

    logits = logits_ref[...]
    lt = logits.T
    m1t = jnp.max(lt, axis=0, keepdims=True)
    m2t = jnp.max(jnp.where(lt == m1t, -jnp.inf, lt), axis=0, keepdims=True)
    chosen_t = lt >= m2t
    upper = (iota((tok, tok), 0) < iota((tok, tok), 1)).astype(F32).astype(BF16)
    before_t = jnp.dot(chosen_t.astype(F32).astype(BF16), upper, preferred_element_type=F32)
    st_own[...] = jnp.where(chosen_t, before_t, -1.0).astype(BF16)

    m1 = jnp.max(logits, axis=1, keepdims=True)
    is1 = logits == m1
    rest = jnp.where(is1, -jnp.inf, logits)
    m2 = jnp.max(rest, axis=1, keepdims=True)
    is2 = rest == m2
    lower = (iota((tok, tok), 1) < iota((tok, tok), 0)).astype(F32).astype(BF16)
    chosen = jnp.logical_or(is1, is2).astype(F32).astype(BF16)
    before = jnp.dot(lower, chosen, preferred_element_type=F32)
    slot_id = iota((tok, nexp), 1).astype(F32) * src_cap + before
    slot1 = jnp.sum(jnp.where(is1, slot_id, 0.0), axis=1, keepdims=True)
    slot2 = jnp.sum(jnp.where(is2, slot_id, 0.0), axis=1, keepdims=True)
    total = jnp.sum(jnp.exp(logits - m1), axis=1, keepdims=True)
    gate1 = 1.0 / total
    gate2 = jnp.exp(m2 - m1) / total

    for r in (2, 3, 1):
        s_remote(r).start()
    for c in range(1, NCH):
        x_local(c).wait()
        x_remote(c, 2).start()
        x_remote(c, 1).start()

    for r in range(1, NREL):
        s_remote(r).wait_recv()
    own_first = pl.multiple_of(me * edev, edev)
    pos = [st_own[pl.ds(own_first, edev), :].astype(F32)] + [st_all[r].astype(F32) for r in range(1, NREL)]
    cnt = [jnp.sum((p >= 0.0).astype(F32), axis=1, keepdims=True) for p in pos]
    expand = (iota((slots, edev), 0) // src_cap == iota((slots, edev), 1)).astype(F32).astype(BF16)
    slot_no = (iota((slots, tok), 0) % src_cap).astype(F32)
    for r in range(NREL):
        ahead = jnp.zeros_like(cnt[0])
        for q in range(NREL):
            if q != r:
                ahead = ahead + cnt[q] * (dev[q] < dev[r]).astype(F32)
        kept = jnp.where(pos[r] + ahead < cap, pos[r], -1.0).astype(BF16)
        dmat[r] = (jnp.dot(expand, kept, preferred_element_type=F32) == slot_no).astype(F32).astype(BF16)

    def gather_chunk(c):
        x_remote(c, 2).wait_recv()
        x_remote(c, 3).start()
        x_remote(c, 1).wait_recv()
        for r in range(NREL):
            if r == 3:
                x_remote(c, 3).wait_recv()
            part = jnp.dot(dmat[r], xall[r, c], preferred_element_type=F32).astype(BF16)
            xg[:, r] = part.reshape(edev, src_cap, ck)

    for c in range(NCH - 1):
        gather_chunk(c)

        def first_phase(j, carry):
            i0 = c * edev + j * PAIR
            for q in range(PAIR):
                w1_copy(i0 + q).wait()
            for q in range(PAIR):
                e = j * PAIR + q
                part = jnp.dot(xg[e].reshape(rows, ck), w1buf[(i0 + q) % NS1], preferred_element_type=F32)
                if c > 0:
                    part = hacc[e] + part
                hacc[e] = part
            for q in range(PAIR):
                w1_copy(i0 + q + NS1).start()
            return carry
        lax.fori_loop(0, edev // PAIR, first_phase, 0)

    last = (NCH - 1) * edev
    gather_chunk(NCH - 1)

    def second_phase(e, carry):
        w1_copy(last + e).wait()
        h = hacc[e] + jnp.dot(xg[e].reshape(rows, ck), w1buf[(last + e) % NS1], preferred_element_type=F32)

        @pl.when(e + NS1 < edev)
        def _():
            w1_copy(last + e + NS1).start()
        hb[...] = jax.nn.gelu(h, approximate=True).astype(BF16)
        w2_copy(e).wait()
        s = e % NS2
        b, q = e // eblk, e % eblk
        first = pl.multiple_of(q * src_cap, src_cap)
        for c in range(NCH):
            cols = pl.ds(c * ck, ck)
            z = jnp.dot(hb[...], w2buf[s, :, cols], preferred_element_type=F32).astype(BF16)
            zs[e, :, cols] = z
            zr[b, pl.ds(first, src_cap), cols] = z[:src_cap]

        @pl.when(e + NS2 < edev)
        def _():
            w2_copy(e + NS2).start()
        for r in (2, 3, 1):
            z_remote(e, r).start()
        return carry
    lax.fori_loop(0, edev, second_phase, 0)

    ncol = NREL * eblk * src_cap
    col = iota((1, ncol), 1)
    rel = col // (eblk * src_cap)
    rx, rc = rel // 2, rel % 2
    owner = 2 * (rx + mx - 2 * rx * mx) + (rc + mc - 2 * rc * mc)
    for b in range(nblk):
        for r in range(1, NREL):
            z_block(b, r).wait_recv()
        slot = ((owner * edev + b * eblk) * src_cap + col % (eblk * src_cap)).astype(F32)
        pick1 = (slot1 == slot).astype(F32).astype(BF16)
        pick2 = (slot2 == slot).astype(F32).astype(BF16)
        for c in range(NCH):
            cols = pl.ds(c * ck, ck)
            zc = zr[b, :, cols]
            mix = (gate1 * jnp.dot(pick1, zc, preferred_element_type=F32)
                   + gate2 * jnp.dot(pick2, zc, preferred_element_type=F32))
            if b > 0:
                mix = acc[:, cols] + mix
            if b < nblk - 1:
                acc[:, cols] = mix
            else:
                out_ref[:, cols] = (xall[0, c].astype(F32) + mix).astype(BF16)

    for r in range(1, NREL):
        s_remote(r).wait_send()
        for c in range(NCH):
            x_remote(c, r).wait_send()
        for b in range(nblk):
            z_block(b, r).wait_send()


def solution(mesh):
    group_size = mesh.shape['ep']
    row_spec = P(('dp', 'ep'), None)
    expert_spec = P('ep', None, None)

    def local_step(x_rows, logits, w_in, w_out):
        tok, d_model = x_rows.shape
        nexp = logits.shape[1]
        edev, _, ff = w_in.shape
        cap = 2 * tok * group_size // nexp
        src_cap = 4 * tok // nexp
        slots = edev * src_cap
        rows = NREL * src_cap
        ck = d_model // NCH
        eblk = 4
        nblk = edev // eblk
        dma = pltpu.SemaphoreType.DMA
        scratch = [
            pltpu.VMEM((NREL, NCH, tok, ck), BF16),
            pltpu.VMEM((nexp, tok), BF16),
            pltpu.VMEM((NREL, edev, tok), BF16),
            pltpu.VMEM((NREL, slots, tok), BF16),
            pltpu.VMEM((edev, NREL, src_cap, ck), BF16),
            pltpu.VMEM((edev, rows, ff), F32),
            pltpu.VMEM((rows, ff), BF16),
            pltpu.VMEM((NS1, ck, ff), BF16),
            pltpu.VMEM((NS2, ff, d_model), BF16),
            pltpu.VMEM((edev, rows, d_model), BF16),
            pltpu.VMEM((nblk, eblk * rows, d_model), BF16),
            pltpu.VMEM((tok, d_model), F32),
            dma((NS1,)), dma((NS2,)), dma((NCH,)),
            dma((NREL - 1, NCH)), dma((NREL - 1, NCH)),
            dma((NREL - 1,)), dma((NREL - 1,)),
            dma((NREL - 1, nblk)), dma((NREL - 1, nblk)),
        ]
        vmem = pl.BlockSpec(memory_space=pltpu.VMEM)
        hbm = pl.BlockSpec(memory_space=pl.ANY)
        return pl.pallas_call(
            functools.partial(moe_kernel, cap),
            out_shape=jax.ShapeDtypeStruct((tok, d_model), BF16),
            in_specs=[hbm, vmem, hbm, hbm],
            out_specs=vmem,
            scratch_shapes=scratch,
            compiler_params=pltpu.CompilerParams(collective_id=0, has_side_effects=True, vmem_limit_bytes=67000000),
        )(x_rows, logits, w_in, w_out)

    return jax.shard_map(local_step, mesh=mesh, in_specs=(row_spec, row_spec, expert_spec, expert_spec),
                         out_specs=row_spec, check_vma=False)
```

```python
import functools

import jax
import jax.numpy as jnp
from jax import lax
from jax.experimental import pallas as pl
from jax.experimental.pallas import tpu as pltpu
from jax.sharding import PartitionSpec as P

BF16 = jnp.bfloat16
F32 = jnp.float32
MESH = pl.DeviceIdType.MESH
NREL = 4
NCH = 4
NS1 = 12
NS2 = 3
PAIR = 2
UNIT = 16
PACKED = (1, 1, 1, 2, 1, 2, 2, 2)
FULL = (2, 2, 2, 2, 2, 2, 2, 2)


def iota(shape, dim):
    return lax.broadcasted_iota(jnp.int32, shape, dim)


def onehot(mask):
    return mask.astype(F32).astype(BF16)


def moe_kernel(cap, units, x_hbm, lt_ref, w1_hbm, w2_hbm, out_ref, flag_ref, xall, st_own, st_all, dmat, xg, hacc, hb,
               w1buf, w2buf, zs, pk, zr, acc, meta_own, meta_in, flag_own, flag_in, w1_sem, w2_sem, xl_sem, xs_sem,
               xr_sem, ss_sem, sr_sem, ms_sem, mr_sem, fs_sem, fr_sem, ps_sem, pr_sem, zs_sem, zr_sem):
    nexp, tok = lt_ref.shape
    edev, d_model, ff = w1_hbm.shape
    src_cap = xg.shape[2]
    slots = edev * src_cap
    ck = d_model // NCH
    rows = NREL * src_cap
    nblk = edev // PAIR
    starts = [sum(units[:b]) for b in range(nblk + 1)]
    total_rows = starts[nblk] * UNIT
    split_blk = nblk - 2
    split = starts[split_blk] * UNIT

    me = lax.axis_index('ep')
    group = lax.axis_index('dp')
    ngroups = lax.axis_size('dp')
    mx, mc = me // 2, me % 2
    dev = [me, 2 * mx + (1 - mc), 2 * (1 - mx) + mc, 2 * (1 - mx) + (1 - mc)]

    def remote(src, dst, send, recv, r):
        return pltpu.make_async_remote_copy(src_ref=src, dst_ref=dst, send_sem=send, recv_sem=recv,
                                            device_id={'ep': dev[r]}, device_id_type=MESH)

    def w1_copy(i):
        c, e = i // edev, i % edev
        k = pl.multiple_of(c * ck, ck)
        s = i % NS1
        return pltpu.make_async_copy(w1_hbm.at[e, pl.ds(k, ck), :], w1buf.at[s], w1_sem.at[s])

    def w2_copy(e):
        s = e % NS2
        return pltpu.make_async_copy(w2_hbm.at[e], w2buf.at[s], w2_sem.at[s])

    def x_local(c):
        return pltpu.make_async_copy(x_hbm.at[:, pl.ds(c * ck, ck)], xall.at[0, c], xl_sem.at[c])

    def x_remote(c, slot):
        return remote(xall.at[2 if slot == 3 else 0, c], xall.at[slot, c], xs_sem.at[slot - 1, c],
                      xr_sem.at[slot - 1, c], 2 if slot == 2 else 1)

    def s_remote(r):
        first = pl.multiple_of(dev[r] * edev, edev)
        return remote(st_own.at[pl.ds(first, edev), :], st_all.at[r], ss_sem.at[r - 1], sr_sem.at[r - 1], r)

    def m_remote(r):
        return remote(meta_own.at[r], meta_in.at[r], ms_sem.at[r - 1], mr_sem.at[r - 1], r)

    def f_remote(k):
        peer = lax.rem(group + k, ngroups)
        return pltpu.make_async_remote_copy(src_ref=flag_own, dst_ref=flag_in.at[k], send_sem=fs_sem.at[k - 1],
                                            recv_sem=fr_sem.at[k - 1], device_id={'dp': peer}, device_id_type=MESH)

    def partner_remote(e):
        first = pl.multiple_of(e * src_cap, src_cap)
        return remote(zs.at[1, pl.ds(first, src_cap), :], zr.at[1, pl.ds(first, src_cap), :], ps_sem.at[0],
                      pr_sem.at[0], 1)

    def partner_all():
        return remote(zr.at[1], zr.at[1], ps_sem.at[0], pr_sem.at[0], 1)

    def pack_remote(r, first, part):
        return remote(pk.at[r - 2, pl.ds(first, UNIT), :], zr.at[r, pl.ds(first, UNIT), :], zs_sem.at[r - 2, part],
                      zr_sem.at[r - 2, part], r)

    def pack_part(r, part):
        span = pl.ds(0, split) if part == 0 else pl.ds(split, total_rows - split)
        ref = zr.at[r, span, :]
        return remote(ref, ref, zs_sem.at[r - 2, part], zr_sem.at[r - 2, part], r)

    barrier = pltpu.get_barrier_semaphore()
    for r in range(1, NREL):
        pl.semaphore_signal(barrier, inc=1, device_id={'ep': dev[r]}, device_id_type=MESH)
    for k in range(1, ngroups):
        pl.semaphore_signal(barrier, inc=1, device_id={'dp': lax.rem(group + k, ngroups)}, device_id_type=MESH)
    for c in range(NCH):
        x_local(c).start()

    def start_w1(i, carry):
        w1_copy(i).start()
        return carry
    lax.fori_loop(0, NS1, start_w1, 0)
    for e in range(NS2):
        w2_copy(e).start()

    for r in (2, 3):
        zs[r] = jnp.zeros(zs.shape[1:], BF16)
    meta_own[...] = jnp.zeros_like(meta_own)
    pl.semaphore_wait(barrier, NREL - 1 + ngroups - 1)
    x_local(0).wait()
    x_remote(0, 2).start()
    x_remote(0, 1).start()

    lt = lt_ref[...]
    m1t = jnp.max(lt, axis=0, keepdims=True)
    m2t = jnp.max(jnp.where(lt == m1t, -jnp.inf, lt), axis=0, keepdims=True)
    chosen_t = lt >= m2t
    upper = onehot(iota((tok, tok), 0) < iota((tok, tok), 1))
    before_t = jnp.dot(onehot(chosen_t), upper, preferred_element_type=F32)
    st_own[...] = jnp.where(chosen_t, before_t, -1.0).astype(BF16)

    logits = lt.T
    m1 = jnp.max(logits, axis=1, keepdims=True)
    is1 = logits == m1
    rest = jnp.where(is1, -jnp.inf, logits)
    m2 = jnp.max(rest, axis=1, keepdims=True)
    is2 = rest == m2
    lower = onehot(iota((tok, tok), 1) < iota((tok, tok), 0))
    before = jnp.dot(lower, onehot(jnp.logical_or(is1, is2)), preferred_element_type=F32)
    total = jnp.sum(jnp.exp(logits - m1), axis=1, keepdims=True)
    gate1 = 1.0 / total
    gate2 = jnp.exp(m2 - m1) / total

    for r in (2, 3, 1):
        s_remote(r).start()
    for c in range(1, NCH):
        x_local(c).wait()
        x_remote(c, 2).start()
        x_remote(c, 1).start()

    for r in range(1, NREL):
        s_remote(r).wait_recv()
    own_first = pl.multiple_of(me * edev, edev)
    pos = [st_own[pl.ds(own_first, edev), :].astype(F32)] + [st_all[r].astype(F32) for r in range(1, NREL)]
    cnt = [jnp.sum((p >= 0.0).astype(F32), axis=1, keepdims=True) for p in pos]
    ahead = []
    for r in range(NREL):
        a = jnp.zeros_like(cnt[0])
        for q in range(NREL):
            if q != r:
                a = a + cnt[q] * (dev[q] < dev[r]).astype(F32)
        ahead.append(a)

    lane_exp = iota((edev, 128), 1) - me * edev == iota((edev, 128), 0)
    exp_no = iota((edev, 1), 0)
    exp_row = exp_no.astype(F32)
    wide = iota((edev, slots), 1)
    own_slot = wide // src_cap == iota((edev, slots), 0)
    over = jnp.zeros((1, 1), F32)
    packed_row = [None, None]
    own_meta = None
    for r in range(NREL):
        if r < 2:
            base = exp_row * src_cap
            rows_kept = jnp.full((edev, 1), float(src_cap), F32)
        else:
            rows_kept = jnp.clip(cap - ahead[r], 0.0, cnt[r])
            base = jnp.zeros((edev, 1), F32)
            end = jnp.zeros((1, 1), F32)
            for b in range(nblk):
                end = jnp.maximum(end, float(starts[b] * UNIT))
                for q in range(PAIR):
                    e = b * PAIR + q
                    base = jnp.where(exp_no == e, end, base)
                    end = end + rows_kept[e:e + 1]
            over = jnp.maximum(over, (end > float(total_rows)).astype(F32))
            row = jnp.where(own_slot, base + (wide % src_cap).astype(F32), 0.0)
            row = jnp.where((wide % src_cap).astype(F32) < rows_kept, row, jnp.where(own_slot, -1.0, 0.0))
            packed_row[r - 2] = jnp.sum(row, axis=0, keepdims=True)
        base_lane = jnp.sum(jnp.where(lane_exp, base + float(r * slots), 0.0), axis=0, keepdims=True)
        kept_lane = jnp.sum(jnp.where(lane_exp, rows_kept, 0.0), axis=0, keepdims=True)
        if r == 0:
            own_meta = (base_lane, kept_lane)
        else:
            meta_own[r, 0:1, :] = base_lane
            meta_own[r, 1:2, :] = kept_lane
    for r in range(1, NREL):
        meta_own[r, 2:3, :] = jnp.broadcast_to(over, (1, 128))

    expand = onehot(iota((slots, edev), 0) // src_cap == iota((slots, edev), 1))
    slot_no = (iota((slots, tok), 0) % src_cap).astype(F32)
    for r in range(NREL):
        kept = jnp.where(pos[r] + ahead[r] < cap, pos[r], -1.0).astype(BF16)
        dmat[r] = onehot(jnp.dot(expand, kept, preferred_element_type=F32) == slot_no)
    for r in (2, 3, 1):
        m_remote(r).start()

    def gather_chunk(c):
        x_remote(c, 2).wait_recv()
        x_remote(c, 3).start()
        x_remote(c, 1).wait_recv()
        for r in range(NREL):
            if r == 3:
                x_remote(c, 3).wait_recv()
            part = jnp.dot(dmat[r], xall[r, c], preferred_element_type=F32).astype(BF16)
            xg[:, r] = part.reshape(edev, src_cap, ck)

    for c in range(NCH - 1):
        gather_chunk(c)

        def first_phase(j, carry):
            i0 = c * edev + j * PAIR
            for q in range(PAIR):
                w1_copy(i0 + q).wait()
            for q in range(PAIR):
                e = j * PAIR + q
                part = jnp.dot(xg[e].reshape(rows, ck), w1buf[(i0 + q) % NS1], preferred_element_type=F32)
                if c > 0:
                    part = hacc[e] + part
                hacc[e] = part
            for q in range(PAIR):
                w1_copy(i0 + q + NS1).start()
            return carry
        lax.fori_loop(0, edev // PAIR, first_phase, 0)

        if c == 0:
            for r in range(1, NREL):
                m_remote(r).wait_recv()
            first_row, kept_rows = own_meta
            for r in range(1, NREL):
                first_row = first_row + meta_in[r, 0:1, :]
                kept_rows = kept_rows + meta_in[r, 1:2, :]
                over = jnp.maximum(over, meta_in[r, 2:3, 0:1])
            flag_own[...] = jnp.broadcast_to(over, flag_own.shape)
            place = jnp.where(before < kept_rows[:, :nexp], first_row[:, :nexp] + before, -1.0)
            slot1 = jnp.sum(jnp.where(is1, place, 0.0), axis=1, keepdims=True)
            slot2 = jnp.sum(jnp.where(is2, place, 0.0), axis=1, keepdims=True)
        if c == 1:
            for k in range(1, ngroups):
                f_remote(k).start()

    last = (NCH - 1) * edev
    gather_chunk(NCH - 1)

    def block(b, carry):
        for q in range(PAIR):
            e = b * PAIR + q
            w1_copy(last + e).wait()
            h = hacc[e] + jnp.dot(xg[e].reshape(rows, ck), w1buf[(last + e) % NS1], preferred_element_type=F32)

            @pl.when(e + NS1 < edev)
            def _():
                w1_copy(last + e + NS1).start()
            hb[...] = jax.nn.gelu(h, approximate=True).astype(BF16)
            w2_copy(e).wait()
            first = pl.multiple_of(e * src_cap, src_cap)
            for c in range(NCH):
                cols = pl.ds(c * ck, ck)
                z = jnp.dot(hb[...], w2buf[e % NS2, :, cols], preferred_element_type=F32).astype(BF16)
                zr[0, pl.ds(first, src_cap), cols] = z[:src_cap]
                for r in range(1, NREL):
                    zs[r, pl.ds(first, src_cap), cols] = z[r * src_cap:(r + 1) * src_cap]

            @pl.when(e + NS2 < edev)
            def _():
                w2_copy(e + NS2).start()
            partner_remote(e).start()
        start = sum((b > j).astype(jnp.int32) * units[j] for j in range(nblk - 1)) * UNIT
        start = pl.multiple_of(start, UNIT)
        double = functools.reduce(jnp.logical_or, [b == j for j in range(nblk) if units[j] == 2])
        part = (b >= split_blk).astype(jnp.int32)
        for r in (2, 3):
            row = (iota((2 * UNIT, slots), 0) + start).astype(F32)
            pick = onehot(row == packed_row[r - 2])
            for c in range(NCH):
                cols = pl.ds(c * ck, ck)
                pk[r - 2, pl.ds(start, 2 * UNIT), cols] = jnp.dot(pick, zs[r, :, cols],
                                                                  preferred_element_type=F32).astype(BF16)
        for r in (2, 3):
            pack_remote(r, start, part).start()

            @pl.when(double)
            def _():
                pack_remote(r, start + UNIT, part).start()
        return carry
    lax.fori_loop(0, nblk, block, 0)

    for k in range(1, ngroups):
        f_remote(k).wait_recv()
    flag = flag_own[...]
    for k in range(1, ngroups):
        flag = jnp.maximum(flag, flag_in[k])
    flag_ref[...] = flag

    pieces = [(0, 0, slots, None), (1, 0, slots, 'partner'), (2, 0, split, 0), (3, 0, split, 0),
              (2, split, total_rows - split, 1), (3, split, total_rows - split, 1)]
    for n, (r, first, size, wait) in enumerate(pieces):
        if wait == 'partner':
            partner_all().wait_recv()
        elif wait is not None:
            pack_part(r, wait).wait_recv()
        slot = (iota((1, size), 1) + (r * slots + first)).astype(F32)
        pick1 = onehot(slot1 == slot)
        pick2 = onehot(slot2 == slot)
        for c in range(NCH):
            cols = pl.ds(c * ck, ck)
            zc = zr[r, first:first + size, cols]
            mix = (gate1 * jnp.dot(pick1, zc, preferred_element_type=F32)
                   + gate2 * jnp.dot(pick2, zc, preferred_element_type=F32))
            if n > 0:
                mix = acc[:, cols] + mix
            if n < len(pieces) - 1:
                acc[:, cols] = mix
            else:
                out_ref[:, cols] = (xall[0, c].astype(F32) + mix).astype(BF16)

    for k in range(1, ngroups):
        f_remote(k).wait_send()
    partner_all().wait_send()
    for r in range(1, NREL):
        s_remote(r).wait_send()
        m_remote(r).wait_send()
        for c in range(NCH):
            x_remote(c, r).wait_send()
        if r >= 2:
            for part in range(2):
                pack_part(r, part).wait_send()


def solution(mesh):
    group_size = mesh.shape['ep']
    ngroups = mesh.shape['dp']
    row_spec = P(('dp', 'ep'), None)
    expert_spec = P('ep', None, None)

    def call(units, collective, x_rows, logits_t, w_in, w_out):
        tok, d_model = x_rows.shape
        nexp = logits_t.shape[0]
        edev, _, ff = w_in.shape
        cap = 2 * tok * group_size // nexp
        src_cap = 4 * tok // nexp
        slots = edev * src_cap
        rows = NREL * src_cap
        ck = d_model // NCH
        dma = pltpu.SemaphoreType.DMA
        scratch = [
            pltpu.VMEM((NREL, NCH, tok, ck), BF16),
            pltpu.VMEM((nexp, tok), BF16),
            pltpu.VMEM((NREL, edev, tok), BF16),
            pltpu.VMEM((NREL, slots, tok), BF16),
            pltpu.VMEM((edev, NREL, src_cap, ck), BF16),
            pltpu.VMEM((edev, rows, ff), F32),
            pltpu.VMEM((rows, ff), BF16),
            pltpu.VMEM((NS1, ck, ff), BF16),
            pltpu.VMEM((NS2, ff, d_model), BF16),
            pltpu.VMEM((NREL, slots, d_model), BF16),
            pltpu.VMEM((2, sum(units) * UNIT, d_model), BF16),
            pltpu.VMEM((NREL, slots, d_model), BF16),
            pltpu.VMEM((tok, d_model), F32),
            pltpu.VMEM((NREL, 8, 128), F32), pltpu.VMEM((NREL, 8, 128), F32),
            pltpu.VMEM((8, 128), F32), pltpu.VMEM((ngroups, 8, 128), F32),
            dma((NS1,)), dma((NS2,)), dma((NCH,)),
            dma((NREL - 1, NCH)), dma((NREL - 1, NCH)),
            dma((NREL - 1,)), dma((NREL - 1,)),
            dma((NREL - 1,)), dma((NREL - 1,)),
            dma((ngroups - 1,)), dma((ngroups - 1,)),
            dma((1,)), dma((1,)),
            dma((2, 2)), dma((2, 2)),
        ]
        vmem = pl.BlockSpec(memory_space=pltpu.VMEM)
        hbm = pl.BlockSpec(memory_space=pl.ANY)
        return pl.pallas_call(
            functools.partial(moe_kernel, cap, units),
            out_shape=(jax.ShapeDtypeStruct((tok, d_model), BF16), jax.ShapeDtypeStruct((8, 128), F32)),
            in_specs=[hbm, vmem, hbm, hbm],
            out_specs=(vmem, vmem),
            scratch_shapes=scratch,
            compiler_params=pltpu.CompilerParams(collective_id=collective, has_side_effects=True,
                                                 vmem_limit_bytes=67000000),
        )(x_rows, logits_t, w_in, w_out)

    def local_step(x_rows, logits, w_in, w_out):
        args = (x_rows, logits.T, w_in, w_out)
        out, flag = call(PACKED, 0, *args)
        return lax.cond(flag[0, 0] > 0.0, lambda: call(FULL, 1, *args)[0], lambda: out)

    return jax.shard_map(local_step, mesh=mesh, in_specs=(row_spec, row_spec, expert_spec, expert_spec),
                         out_specs=row_spec, check_vma=False)
```

```python
import functools

import jax
import jax.numpy as jnp
from jax import lax
from jax.experimental import pallas as pl
from jax.experimental.pallas import tpu as pltpu
from jax.sharding import PartitionSpec as P

BF16 = jnp.bfloat16
F32 = jnp.float32
MESH = pl.DeviceIdType.MESH
NREL = 4
NCH = 4
NS1 = 14
NS2 = 3
STEP = 4
UNIT = 16
TAIL = 2
PACKED = (0, 1, 1, 0, 1, 0, 1, 0, 1, 1, 1, 1, 1, 1, 1, 1)
FULL = (1,) * 16


def iota(shape, dim):
    return lax.broadcasted_iota(jnp.int32, shape, dim)


def onehot(mask):
    return mask.astype(F32).astype(BF16)


def moe_kernel(cap, units, x_hbm, lt_ref, w1_hbm, w2_hbm, out_ref, flag_ref, xall, st_own, st_all, dmat, xg, hacc, hb,
               w1buf, w2buf, zs, pk, zr, meta_own, meta_in, flag_own, flag_in, choice, w1_sem, w2_sem, xl_sem, xs_sem,
               xr_sem, ss_sem, sr_sem, ms_sem, mr_sem, fs_sem, fr_sem, ps_sem, pr_sem, zs_sem, zr_sem):
    nexp, tok = lt_ref.shape
    edev, d_model, ff = w1_hbm.shape
    src_cap = xg.shape[2]
    slots = edev * src_cap
    ck = d_model // NCH
    rows = NREL * src_cap
    total_rows = sum(units) * UNIT
    split = total_rows - TAIL * UNIT

    me = lax.axis_index('ep')
    group = lax.axis_index('dp')
    ngroups = lax.axis_size('dp')
    mx, mc = me // 2, me % 2
    dev = [me, 2 * mx + (1 - mc), 2 * (1 - mx) + mc, 2 * (1 - mx) + (1 - mc)]

    def remote(src, dst, send, recv, r):
        return pltpu.make_async_remote_copy(src_ref=src, dst_ref=dst, send_sem=send, recv_sem=recv,
                                            device_id={'ep': dev[r]}, device_id_type=MESH)

    def w1_copy(i):
        c, e = i // edev, i % edev
        k = pl.multiple_of(c * ck, ck)
        s = i % NS1
        return pltpu.make_async_copy(w1_hbm.at[e, pl.ds(k, ck), :], w1buf.at[s], w1_sem.at[s])

    def w2_copy(e):
        s = e % NS2
        return pltpu.make_async_copy(w2_hbm.at[e], w2buf.at[s], w2_sem.at[s])

    def x_local(c):
        return pltpu.make_async_copy(x_hbm.at[:, pl.ds(c * ck, ck)], xall.at[0, c], xl_sem.at[c])

    def x_remote(c, slot):
        return remote(xall.at[2 if slot == 3 else 0, c], xall.at[slot, c], xs_sem.at[slot - 1, c],
                      xr_sem.at[slot - 1, c], 2 if slot == 2 else 1)

    def s_remote(r):
        first = pl.multiple_of(dev[r] * edev, edev)
        return remote(st_own.at[pl.ds(first, edev), :], st_all.at[r], ss_sem.at[r - 1], sr_sem.at[r - 1], r)

    def m_remote(r):
        return remote(meta_own.at[r], meta_in.at[r], ms_sem.at[r - 1], mr_sem.at[r - 1], r)

    def f_remote(k):
        peer = lax.rem(group + k, ngroups)
        return pltpu.make_async_remote_copy(src_ref=flag_own, dst_ref=flag_in.at[k], send_sem=fs_sem.at[k - 1],
                                            recv_sem=fr_sem.at[k - 1], device_id={'dp': peer}, device_id_type=MESH)

    def partner_remote(e):
        first = pl.multiple_of(e * src_cap, src_cap)
        return remote(zs.at[0, pl.ds(first, src_cap), :], zr.at[1, pl.ds(first, src_cap), :], ps_sem.at[0],
                      pr_sem.at[0], 1)

    def partner_all():
        return remote(zr.at[1], zr.at[1], ps_sem.at[0], pr_sem.at[0], 1)

    def pack_remote(r, first, part):
        return remote(pk.at[r - 2, pl.ds(first, UNIT), :], zr.at[r, pl.ds(first, UNIT), :], zs_sem.at[r - 2, part],
                      zr_sem.at[r - 2, part], r)

    def pack_part(r, part):
        span = pl.ds(0, split) if part == 0 else pl.ds(split, total_rows - split)
        ref = zr.at[r, span, :]
        return remote(ref, ref, zs_sem.at[r - 2, part], zr_sem.at[r - 2, part], r)

    barrier = pltpu.get_barrier_semaphore()
    for r in range(1, NREL):
        pl.semaphore_signal(barrier, inc=1, device_id={'ep': dev[r]}, device_id_type=MESH)
    for k in range(1, ngroups):
        pl.semaphore_signal(barrier, inc=1, device_id={'dp': lax.rem(group + k, ngroups)}, device_id_type=MESH)
    for c in range(NCH):
        x_local(c).start()

    def start_w1(i, carry):
        w1_copy(i).start()
        return carry
    lax.fori_loop(0, NS1, start_w1, 0)
    for e in range(NS2):
        w2_copy(e).start()

    for r in (2, 3):
        zs[r - 1] = jnp.zeros(zs.shape[1:], BF16)
    meta_own[...] = jnp.zeros_like(meta_own)

    lt = lt_ref[...]
    m1t = jnp.max(lt, axis=0, keepdims=True)
    m2t = jnp.max(jnp.where(lt == m1t, -jnp.inf, lt), axis=0, keepdims=True)
    chosen_t = lt >= m2t
    upper = onehot(iota((tok, tok), 0) < iota((tok, tok), 1))
    before_t = jnp.dot(onehot(chosen_t), upper, preferred_element_type=F32)
    st_own[...] = jnp.where(chosen_t, before_t, -1.0).astype(BF16)

    pl.semaphore_wait(barrier, NREL - 1 + ngroups - 1)
    for r in (2, 3, 1):
        s_remote(r).start()
    for c in range(NCH):
        x_local(c).wait()
        x_remote(c, 2).start()
        x_remote(c, 1).start()

    logits = lt.T
    m1 = jnp.max(logits, axis=1, keepdims=True)
    is1 = logits == m1
    rest = jnp.where(is1, -jnp.inf, logits)
    m2 = jnp.max(rest, axis=1, keepdims=True)
    is2 = rest == m2
    lower = onehot(iota((tok, tok), 1) < iota((tok, tok), 0))
    before = jnp.dot(lower, onehot(jnp.logical_or(is1, is2)), preferred_element_type=F32)
    total = jnp.sum(jnp.exp(logits - m1), axis=1, keepdims=True)
    gate1 = 1.0 / total
    gate2 = jnp.exp(m2 - m1) / total

    for r in range(1, NREL):
        s_remote(r).wait_recv()
    own_first = pl.multiple_of(me * edev, edev)
    pos = [st_own[pl.ds(own_first, edev), :].astype(F32)] + [st_all[r].astype(F32) for r in range(1, NREL)]
    cnt = [jnp.sum((p >= 0.0).astype(F32), axis=1, keepdims=True) for p in pos]
    ahead = []
    for r in range(NREL):
        a = jnp.zeros_like(cnt[0])
        for q in range(NREL):
            if q != r:
                a = a + cnt[q] * (dev[q] < dev[r]).astype(F32)
        ahead.append(a)

    lane_exp = iota((edev, 128), 1) - me * edev == iota((edev, 128), 0)
    exp_no = iota((edev, 1), 0)
    exp_row = exp_no.astype(F32)
    wide = iota((edev, slots), 1)
    own_slot = wide // src_cap == iota((edev, slots), 0)
    over = jnp.zeros((1, 1), F32)
    packed_row = [None, None]
    own_meta = None
    for r in range(NREL):
        if r < 2:
            base = exp_row * src_cap
            rows_kept = jnp.full((edev, 1), float(src_cap), F32)
        else:
            rows_kept = jnp.clip(cap - ahead[r], 0.0, cnt[r])
            base = jnp.zeros((edev, 1), F32)
            end = jnp.zeros((1, 1), F32)
            for e in range(edev):
                end = jnp.maximum(end, float(sum(units[:e]) * UNIT))
                base = jnp.where(exp_no == e, end, base)
                end = end + rows_kept[e:e + 1]
            over = jnp.maximum(over, (end > float(total_rows)).astype(F32))
            row = jnp.where(own_slot, base + (wide % src_cap).astype(F32), 0.0)
            row = jnp.where((wide % src_cap).astype(F32) < rows_kept, row, jnp.where(own_slot, -1.0, 0.0))
            packed_row[r - 2] = jnp.sum(row, axis=0, keepdims=True)
        base_lane = jnp.sum(jnp.where(lane_exp, base + float(r * slots), 0.0), axis=0, keepdims=True)
        kept_lane = jnp.sum(jnp.where(lane_exp, rows_kept, 0.0), axis=0, keepdims=True)
        if r == 0:
            own_meta = (base_lane, kept_lane)
        else:
            meta_own[r, 0:1, :] = base_lane
            meta_own[r, 1:2, :] = kept_lane
    for r in range(1, NREL):
        meta_own[r, 2:3, :] = jnp.broadcast_to(over, (1, 128))

    expand = onehot(iota((slots, edev), 0) // src_cap == iota((slots, edev), 1))
    slot_no = (iota((slots, tok), 0) % src_cap).astype(F32)
    for r in range(NREL):
        kept = jnp.where(pos[r] + ahead[r] < cap, pos[r], -1.0).astype(BF16)
        dmat[r] = onehot(jnp.dot(expand, kept, preferred_element_type=F32) == slot_no)
    for r in (2, 3, 1):
        m_remote(r).start()

    def gather_chunk(c):
        x_remote(c, 2).wait_recv()
        x_remote(c, 3).start()
        x_remote(c, 1).wait_recv()
        for r in range(NREL):
            if r == 3:
                x_remote(c, 3).wait_recv()
            part = jnp.dot(dmat[r], xall[r, c], preferred_element_type=F32).astype(BF16)
            xg[:, r] = part.reshape(edev, src_cap, ck)

    for c in range(NCH - 1):
        gather_chunk(c)

        def first_phase(j, carry):
            i0 = c * edev + j * STEP
            for q in range(STEP):
                w1_copy(i0 + q).wait()
            for q in range(STEP):
                e = j * STEP + q
                part = jnp.dot(xg[e].reshape(rows, ck), w1buf[(i0 + q) % NS1], preferred_element_type=F32)
                if c > 0:
                    part = hacc[e] + part
                hacc[e] = part
            for q in range(STEP):
                w1_copy(i0 + q + NS1).start()
            return carry
        lax.fori_loop(0, edev // STEP, first_phase, 0)

    last = (NCH - 1) * edev
    gather_chunk(NCH - 1)

    def place_rows():
        for r in range(1, NREL):
            m_remote(r).wait_recv()
        first_row, kept_rows = own_meta
        flag = over
        for r in range(1, NREL):
            first_row = first_row + meta_in[r, 0:1, :]
            kept_rows = kept_rows + meta_in[r, 1:2, :]
            flag = jnp.maximum(flag, meta_in[r, 2:3, 0:1])
        flag_own[...] = jnp.broadcast_to(flag, flag_own.shape)
        place = jnp.where(before < kept_rows[:, :nexp], first_row[:, :nexp] + before, -1.0)
        choice[:, 0:1] = jnp.sum(jnp.where(is1, place, 0.0), axis=1, keepdims=True)
        choice[:, 1:2] = jnp.sum(jnp.where(is2, place, 0.0), axis=1, keepdims=True)

    def second_phase(e, carry):
        @pl.when(e == edev // 4)
        def _():
            place_rows()

        @pl.when(e == edev // 2)
        def _():
            for k in range(1, ngroups):
                f_remote(k).start()
        w1_copy(last + e).wait()
        h = hacc[e] + jnp.dot(xg[e].reshape(rows, ck), w1buf[(last + e) % NS1], preferred_element_type=F32)

        @pl.when(e + NS1 < edev)
        def _():
            w1_copy(last + e + NS1).start()
        hb[...] = jax.nn.gelu(h, approximate=True).astype(BF16)
        w2_copy(e).wait()
        first = pl.multiple_of(e * src_cap, src_cap)
        for c in range(NCH):
            cols = pl.ds(c * ck, ck)
            z = jnp.dot(hb[...], w2buf[e % NS2, :, cols], preferred_element_type=F32).astype(BF16)
            zr[0, pl.ds(first, src_cap), cols] = z[:src_cap]
            for r in range(1, NREL):
                zs[r - 1, pl.ds(first, src_cap), cols] = z[r * src_cap:(r + 1) * src_cap]

        @pl.when(e + NS2 < edev)
        def _():
            w2_copy(e + NS2).start()

        @pl.when(functools.reduce(jnp.logical_or, [e == j for j in range(edev) if units[j]]))
        def _():
            start = sum((e > j).astype(jnp.int32) for j in range(edev - 1) if units[j]) * UNIT
            start = pl.multiple_of(start, UNIT)
            for r in (2, 3):
                row = (iota((UNIT, slots), 0) + start).astype(F32)
                pick = onehot(row == packed_row[r - 2])
                for c in range(NCH):
                    cols = pl.ds(c * ck, ck)
                    pk[r - 2, pl.ds(start, UNIT), cols] = jnp.dot(pick, zs[r - 1, :, cols],
                                                                  preferred_element_type=F32).astype(BF16)
            for r in (2, 3):
                pack_remote(r, start, (start >= split).astype(jnp.int32)).start()
        partner_remote(e).start()
        return carry
    lax.fori_loop(0, edev, second_phase, 0)

    for k in range(1, ngroups):
        f_remote(k).wait_recv()
    flag = flag_own[...]
    for k in range(1, ngroups):
        flag = jnp.maximum(flag, flag_in[k])
    flag_ref[...] = flag

    slot1, slot2 = choice[:, 0:1], choice[:, 1:2]
    far = total_rows - split
    pieces = [((0,), 0, slots), ((1,), 0, slots), ((2, 3), 0, split), ((2, 3), split, far)]
    for n, (rels, first, size) in enumerate(pieces):
        for r in rels:
            if r == 1:
                partner_all().wait_recv()
            elif r >= 2:
                pack_part(r, n - 2).wait_recv()
        slot = jnp.concatenate([(iota((1, size), 1) + (r * slots + first)).astype(F32) for r in rels], axis=1)
        pick1 = onehot(slot1 == slot)
        pick2 = onehot(slot2 == slot)
        for c in range(NCH):
            cols = pl.ds(c * ck, ck)
            zc = jnp.concatenate([zr[r, first:first + size, cols] for r in rels], axis=0)
            mix = (gate1 * jnp.dot(pick1, zc, preferred_element_type=F32)
                   + gate2 * jnp.dot(pick2, zc, preferred_element_type=F32))
            if n > 0:
                mix = out_ref[:, cols] + mix
            out_ref[:, cols] = mix

    for k in range(1, ngroups):
        f_remote(k).wait_send()
    partner_all().wait_send()
    for r in range(1, NREL):
        s_remote(r).wait_send()
        m_remote(r).wait_send()
        for c in range(NCH):
            x_remote(c, r).wait_send()
        if r >= 2:
            for part in range(2):
                pack_part(r, part).wait_send()


def solution(mesh):
    group_size = mesh.shape['ep']
    ngroups = mesh.shape['dp']
    row_spec = P(('dp', 'ep'), None)
    expert_spec = P('ep', None, None)

    def call(units, collective, x_rows, logits_t, w_in, w_out):
        tok, d_model = x_rows.shape
        nexp = logits_t.shape[0]
        edev, _, ff = w_in.shape
        cap = 2 * tok * group_size // nexp
        src_cap = 4 * tok // nexp
        slots = edev * src_cap
        rows = NREL * src_cap
        ck = d_model // NCH
        dma = pltpu.SemaphoreType.DMA
        scratch = [
            pltpu.VMEM((NREL, NCH, tok, ck), BF16),
            pltpu.VMEM((nexp, tok), BF16),
            pltpu.VMEM((NREL, edev, tok), BF16),
            pltpu.VMEM((NREL, slots, tok), BF16),
            pltpu.VMEM((edev, NREL, src_cap, ck), BF16),
            pltpu.VMEM((edev, rows, ff), F32),
            pltpu.VMEM((rows, ff), BF16),
            pltpu.VMEM((NS1, ck, ff), BF16),
            pltpu.VMEM((NS2, ff, d_model), BF16),
            pltpu.VMEM((NREL - 1, slots, d_model), BF16),
            pltpu.VMEM((2, sum(units) * UNIT, d_model), BF16),
            pltpu.VMEM((NREL, slots, d_model), BF16),
            pltpu.VMEM((NREL, 8, 128), F32), pltpu.VMEM((NREL, 8, 128), F32),
            pltpu.VMEM((8, 128), F32), pltpu.VMEM((ngroups, 8, 128), F32), pltpu.VMEM((tok, 128), F32),
            dma((NS1,)), dma((NS2,)), dma((NCH,)),
            dma((NREL - 1, NCH)), dma((NREL - 1, NCH)),
            dma((NREL - 1,)), dma((NREL - 1,)),
            dma((NREL - 1,)), dma((NREL - 1,)),
            dma((ngroups - 1,)), dma((ngroups - 1,)),
            dma((1,)), dma((1,)),
            dma((2, 2)), dma((2, 2)),
        ]
        vmem = pl.BlockSpec(memory_space=pltpu.VMEM)
        hbm = pl.BlockSpec(memory_space=pl.ANY)
        return pl.pallas_call(
            functools.partial(moe_kernel, cap, units),
            out_shape=(jax.ShapeDtypeStruct((tok, d_model), F32), jax.ShapeDtypeStruct((8, 128), F32)),
            in_specs=[hbm, vmem, hbm, hbm],
            out_specs=(vmem, vmem),
            scratch_shapes=scratch,
            compiler_params=pltpu.CompilerParams(collective_id=collective, has_side_effects=True,
                                                 vmem_limit_bytes=67000000),
        )(x_rows, logits_t, w_in, w_out)

    def local_step(x_rows, logits, w_in, w_out):
        args = (x_rows, logits.T, w_in, w_out)
        mix, flag = call(PACKED, 0, *args)
        mix = lax.cond(flag[0, 0] > 0.0, lambda: call(FULL, 1, *args)[0], lambda: mix)
        return (x_rows.astype(F32) + mix).astype(BF16)

    return jax.shard_map(local_step, mesh=mesh, in_specs=(row_spec, row_spec, expert_spec, expert_spec),
                         out_specs=row_spec, check_vma=False)
```

```python
import functools

import jax
import jax.numpy as jnp
from jax import lax
from jax.experimental import pallas as pl
from jax.experimental.pallas import tpu as pltpu
from jax.sharding import PartitionSpec as P

BF16 = jnp.bfloat16
F32 = jnp.float32
MESH = pl.DeviceIdType.MESH
NREL = 4
NCH = 4
NS1 = 14
NS2 = 3
STEP = 4
UNIT = 16
TAIL = 2
PACKED = (0, 1, 1, 0, 1, 0, 1, 0, 1, 1, 1, 1, 1, 1, 1, 1)
FULL = (1,) * 16


def iota(shape, dim):
    return lax.broadcasted_iota(jnp.int32, shape, dim)


def onehot(mask):
    return mask.astype(F32).astype(BF16)


def moe_kernel(cap, units, x_hbm, lt_ref, w1_hbm, w2_hbm, out_ref, flag_ref, xall, st_own, st_all, dmat, xg, hacc, hb0, hb1,
               w1buf, w2buf, zs, pk, zr, acc, meta_own, meta_in, flag_own, flag_in, choice, w1_sem, w2_sem, xl_sem, xs_sem,
               xr_sem, ss_sem, sr_sem, ms_sem, mr_sem, fs_sem, fr_sem, ps_sem, pr_sem, zs_sem, zr_sem):
    nexp, tok = lt_ref.shape
    edev, d_model, ff = w1_hbm.shape
    src_cap = xg.shape[2]
    slots = edev * src_cap
    ck = d_model // NCH
    rows = NREL * src_cap
    total_rows = sum(units) * UNIT
    split = total_rows - TAIL * UNIT

    me = lax.axis_index('ep')
    group = lax.axis_index('dp')
    ngroups = lax.axis_size('dp')
    mx, mc = me // 2, me % 2
    dev = [me, 2 * mx + (1 - mc), 2 * (1 - mx) + mc, 2 * (1 - mx) + (1 - mc)]

    def remote(src, dst, send, recv, r):
        return pltpu.make_async_remote_copy(src_ref=src, dst_ref=dst, send_sem=send, recv_sem=recv,
                                            device_id={'ep': dev[r]}, device_id_type=MESH)

    def w1_copy(i):
        c, e = i // edev, i % edev
        k = pl.multiple_of(c * ck, ck)
        s = i % NS1
        return pltpu.make_async_copy(w1_hbm.at[e, pl.ds(k, ck), :], w1buf.at[s], w1_sem.at[s])

    def w2_copy(e):
        s = e % NS2
        return pltpu.make_async_copy(w2_hbm.at[e], w2buf.at[s], w2_sem.at[s])

    def x_local(c):
        return pltpu.make_async_copy(x_hbm.at[:, pl.ds(c * ck, ck)], xall.at[0, c], xl_sem.at[c])

    def x_remote(c, slot):
        return remote(xall.at[2 if slot == 3 else 0, c], xall.at[slot, c], xs_sem.at[slot - 1, c],
                      xr_sem.at[slot - 1, c], 2 if slot == 2 else 1)

    def s_remote(r):
        first = pl.multiple_of(dev[r] * edev, edev)
        return remote(st_own.at[pl.ds(first, edev), :], st_all.at[r], ss_sem.at[r - 1], sr_sem.at[r - 1], r)

    def m_remote(r):
        return remote(meta_own.at[r], meta_in.at[r], ms_sem.at[r - 1], mr_sem.at[r - 1], r)

    def f_remote(k):
        peer = lax.rem(group + k, ngroups)
        return pltpu.make_async_remote_copy(src_ref=flag_own, dst_ref=flag_in.at[k], send_sem=fs_sem.at[k - 1],
                                            recv_sem=fr_sem.at[k - 1], device_id={'dp': peer}, device_id_type=MESH)

    def partner_remote(e):
        first = pl.multiple_of(e * src_cap, src_cap)
        return remote(zs.at[0, pl.ds(first, src_cap), :], zr.at[1, pl.ds(first, src_cap), :], ps_sem.at[0],
                      pr_sem.at[0], 1)

    def partner_all():
        return remote(zr.at[1], zr.at[1], ps_sem.at[0], pr_sem.at[0], 1)

    def pack_remote(r, first, part):
        return remote(pk.at[r - 2, pl.ds(first, UNIT), :], zr.at[r, pl.ds(first, UNIT), :], zs_sem.at[r - 2, part],
                      zr_sem.at[r - 2, part], r)

    def pack_part(r, part):
        span = pl.ds(0, split) if part == 0 else pl.ds(split, total_rows - split)
        ref = zr.at[r, span, :]
        return remote(ref, ref, zs_sem.at[r - 2, part], zr_sem.at[r - 2, part], r)

    barrier = pltpu.get_barrier_semaphore()
    for r in range(1, NREL):
        pl.semaphore_signal(barrier, inc=1, device_id={'ep': dev[r]}, device_id_type=MESH)
    for k in range(1, ngroups):
        pl.semaphore_signal(barrier, inc=1, device_id={'dp': lax.rem(group + k, ngroups)}, device_id_type=MESH)
    for c in range(NCH):
        x_local(c).start()

    def start_w1(i, carry):
        w1_copy(i).start()
        return carry
    lax.fori_loop(0, NS1, start_w1, 0)
    for e in range(NS2):
        w2_copy(e).start()

    for r in (2, 3):
        zs[r - 1] = jnp.zeros(zs.shape[1:], BF16)
    meta_own[...] = jnp.zeros_like(meta_own)

    lt = lt_ref[...]
    m1t = jnp.max(lt, axis=0, keepdims=True)
    m2t = jnp.max(jnp.where(lt == m1t, -jnp.inf, lt), axis=0, keepdims=True)
    chosen_t = lt >= m2t
    upper = onehot(iota((tok, tok), 0) < iota((tok, tok), 1))
    before_t = jnp.dot(onehot(chosen_t), upper, preferred_element_type=F32)
    st_own[...] = jnp.where(chosen_t, before_t, -1.0).astype(BF16)

    pl.semaphore_wait(barrier, NREL - 1 + ngroups - 1)
    for r in (2, 3, 1):
        s_remote(r).start()
    for c in range(NCH):
        x_local(c).wait()
        x_remote(c, 2).start()
        x_remote(c, 1).start()

    logits = lt.T
    m1 = jnp.max(logits, axis=1, keepdims=True)
    is1 = logits == m1
    rest = jnp.where(is1, -jnp.inf, logits)
    m2 = jnp.max(rest, axis=1, keepdims=True)
    is2 = rest == m2
    lower = onehot(iota((tok, tok), 1) < iota((tok, tok), 0))
    before = jnp.dot(lower, onehot(jnp.logical_or(is1, is2)), preferred_element_type=F32)
    total = jnp.sum(jnp.exp(logits - m1), axis=1, keepdims=True)
    gate1 = 1.0 / total
    gate2 = jnp.exp(m2 - m1) / total

    for r in range(1, NREL):
        s_remote(r).wait_recv()
    own_first = pl.multiple_of(me * edev, edev)
    pos = [st_own[pl.ds(own_first, edev), :].astype(F32)] + [st_all[r].astype(F32) for r in range(1, NREL)]
    cnt = [jnp.sum((p >= 0.0).astype(F32), axis=1, keepdims=True) for p in pos]
    ahead = []
    for r in range(NREL):
        a = jnp.zeros_like(cnt[0])
        for q in range(NREL):
            if q != r:
                a = a + cnt[q] * (dev[q] < dev[r]).astype(F32)
        ahead.append(a)

    lane_exp = iota((edev, 128), 1) - me * edev == iota((edev, 128), 0)
    exp_no = iota((edev, 1), 0)
    exp_row = exp_no.astype(F32)
    wide = iota((edev, slots), 1)
    own_slot = wide // src_cap == iota((edev, slots), 0)
    over = jnp.zeros((1, 1), F32)
    packed_row = [None, None]
    own_meta = None
    for r in range(NREL):
        if r < 2:
            base = exp_row * src_cap
            rows_kept = jnp.full((edev, 1), float(src_cap), F32)
        else:
            rows_kept = jnp.clip(cap - ahead[r], 0.0, cnt[r])
            base = jnp.zeros((edev, 1), F32)
            end = jnp.zeros((1, 1), F32)
            for e in range(edev):
                end = jnp.maximum(end, float(sum(units[:e]) * UNIT))
                base = jnp.where(exp_no == e, end, base)
                end = end + rows_kept[e:e + 1]
            over = jnp.maximum(over, (end > float(total_rows)).astype(F32))
            row = jnp.where(own_slot, base + (wide % src_cap).astype(F32), 0.0)
            row = jnp.where((wide % src_cap).astype(F32) < rows_kept, row, jnp.where(own_slot, -1.0, 0.0))
            packed_row[r - 2] = jnp.sum(row, axis=0, keepdims=True)
        base_lane = jnp.sum(jnp.where(lane_exp, base + float(r * slots), 0.0), axis=0, keepdims=True)
        kept_lane = jnp.sum(jnp.where(lane_exp, rows_kept, 0.0), axis=0, keepdims=True)
        if r == 0:
            own_meta = (base_lane, kept_lane)
        else:
            meta_own[r, 0:1, :] = base_lane
            meta_own[r, 1:2, :] = kept_lane
    for r in range(1, NREL):
        meta_own[r, 2:3, :] = jnp.broadcast_to(over, (1, 128))

    expand = onehot(iota((slots, edev), 0) // src_cap == iota((slots, edev), 1))
    slot_no = (iota((slots, tok), 0) % src_cap).astype(F32)
    for r in range(NREL):
        kept = jnp.where(pos[r] + ahead[r] < cap, pos[r], -1.0).astype(BF16)
        dmat[r] = onehot(jnp.dot(expand, kept, preferred_element_type=F32) == slot_no)
    for r in (2, 3, 1):
        m_remote(r).start()

    def relay(c):
        x_remote(c, 2).wait_recv()
        x_remote(c, 3).start()

    def gather_chunk(c):
        if c < 2:
            relay(c)
        x_remote(c, 1).wait_recv()
        for r in range(NREL):
            if r == 3:
                x_remote(c, 3).wait_recv()
            part = jnp.dot(dmat[r], xall[r, c], preferred_element_type=F32).astype(BF16)
            xg[:, r] = part.reshape(edev, src_cap, ck)

    for c in range(NCH - 1):
        gather_chunk(c)

        def first_phase(j, carry):
            if c > 0:
                @pl.when(j == edev // STEP - 1)
                def _():
                    relay(c + 1)
            i0 = c * edev + j * STEP
            for q in range(STEP):
                w1_copy(i0 + q).wait()
            for q in range(STEP):
                e = j * STEP + q
                part = jnp.dot(xg[e].reshape(rows, ck), w1buf[(i0 + q) % NS1], preferred_element_type=F32)
                if c > 0:
                    part = hacc[e] + part
                hacc[e] = part
            for q in range(STEP):
                w1_copy(i0 + q + NS1).start()
            return carry
        lax.fori_loop(0, edev // STEP, first_phase, 0)

    last = (NCH - 1) * edev
    gather_chunk(NCH - 1)

    def place_rows():
        for r in range(1, NREL):
            m_remote(r).wait_recv()
        first_row, kept_rows = own_meta
        flag = over
        for r in range(1, NREL):
            first_row = first_row + meta_in[r, 0:1, :]
            kept_rows = kept_rows + meta_in[r, 1:2, :]
            flag = jnp.maximum(flag, meta_in[r, 2:3, 0:1])
        flag_own[...] = jnp.broadcast_to(flag, flag_own.shape)
        place = jnp.where(before < kept_rows[:, :nexp], first_row[:, :nexp] + before, -1.0)
        choice[:, 0:1] = jnp.sum(jnp.where(is1, place, 0.0), axis=1, keepdims=True)
        choice[:, 1:2] = jnp.sum(jnp.where(is2, place, 0.0), axis=1, keepdims=True)

    def first_product(e, hidden):
        h = hacc[e] + jnp.dot(xg[e].reshape(rows, ck), w1buf[(last + e) % NS1], preferred_element_type=F32)
        hidden[...] = jax.nn.gelu(h, approximate=True).astype(BF16)

    def send_packed(e):
        start = sum((e > j).astype(jnp.int32) for j in range(edev - 1) if units[j]) * UNIT
        start = pl.multiple_of(start, UNIT)
        for r in (2, 3):
            row = (iota((UNIT, slots), 0) + start).astype(F32)
            pick = onehot(row == packed_row[r - 2])
            for c in range(NCH):
                cols = pl.ds(c * ck, ck)
                pk[r - 2, pl.ds(start, UNIT), cols] = jnp.dot(pick, zs[r - 1, :, cols],
                                                              preferred_element_type=F32).astype(BF16)
        for r in (2, 3):
            pack_remote(r, start, (start >= split).astype(jnp.int32)).start()

    def expert(e, hidden, following):
        if following is not None:
            w1_copy(last + e + 1).wait()
        w2_copy(e).wait()
        if following is not None:
            first_product(e + 1, following)
        first = pl.multiple_of(e * src_cap, src_cap)
        for c in range(NCH):
            cols = pl.ds(c * ck, ck)
            z = jnp.dot(hidden[...], w2buf[e % NS2, :, cols], preferred_element_type=F32).astype(BF16)
            zr[0, pl.ds(first, src_cap), cols] = z[:src_cap]
            for r in range(1, NREL):
                zs[r - 1, pl.ds(first, src_cap), cols] = z[r * src_cap:(r + 1) * src_cap]

        @pl.when(e + NS2 < edev)
        def _():
            w2_copy(e + NS2).start()

        @pl.when(e + 1 + NS1 < edev)
        def _():
            w1_copy(last + e + 1 + NS1).start()

        @pl.when(functools.reduce(jnp.logical_or, [e == j for j in range(edev) if units[j]]))
        def _():
            send_packed(e)
        partner_remote(e).start()

    w1_copy(last).wait()
    first_product(0, hb0)
    if NS1 < edev:
        w1_copy(last + NS1).start()

    def second_phase(j, carry):
        @pl.when(j == 2)
        def _():
            place_rows()

        @pl.when(j == 4)
        def _():
            for k in range(1, ngroups):
                f_remote(k).start()
        expert(2 * j, hb0, hb1)
        expert(2 * j + 1, hb1, hb0)
        return carry
    lax.fori_loop(0, edev // 2 - 1, second_phase, 0)
    expert(jnp.int32(edev - 2), hb0, hb1)
    expert(jnp.int32(edev - 1), hb1, None)

    for k in range(1, ngroups):
        f_remote(k).wait_recv()
    flag = flag_own[...]
    for k in range(1, ngroups):
        flag = jnp.maximum(flag, flag_in[k])
    flag_ref[0] = (jnp.max(flag) > 0.0).astype(jnp.int32)

    slot1, slot2 = choice[:, 0:1], choice[:, 1:2]
    far = total_rows - split
    pieces = [((0,), 0, slots), ((1,), 0, slots), ((2, 3), 0, split), ((2, 3), split, far)]
    for n, (rels, first, size) in enumerate(pieces):
        for r in rels:
            if r == 1:
                partner_all().wait_recv()
            elif r >= 2:
                pack_part(r, n - 2).wait_recv()
        slot = jnp.concatenate([(iota((1, size), 1) + (r * slots + first)).astype(F32) for r in rels], axis=1)
        pick1 = onehot(slot1 == slot)
        pick2 = onehot(slot2 == slot)
        for c in range(NCH):
            cols = pl.ds(c * ck, ck)
            zc = jnp.concatenate([zr[r, first:first + size, cols] for r in rels], axis=0)
            mix = (gate1 * jnp.dot(pick1, zc, preferred_element_type=F32)
                   + gate2 * jnp.dot(pick2, zc, preferred_element_type=F32))
            if n > 0:
                mix = acc[:, cols] + mix
            if n < len(pieces) - 1:
                acc[:, cols] = mix
            else:
                out_ref[:, cols] = (xall[0, c].astype(F32) + mix).astype(BF16)

    for k in range(1, ngroups):
        f_remote(k).wait_send()
    partner_all().wait_send()
    for r in range(1, NREL):
        s_remote(r).wait_send()
        m_remote(r).wait_send()
        for c in range(NCH):
            x_remote(c, r).wait_send()
        if r >= 2:
            for part in range(2):
                pack_part(r, part).wait_send()


def solution(mesh):
    group_size = mesh.shape['ep']
    ngroups = mesh.shape['dp']
    row_spec = P(('dp', 'ep'), None)
    expert_spec = P('ep', None, None)

    def call(units, collective, x_rows, logits_t, w_in, w_out):
        tok, d_model = x_rows.shape
        nexp = logits_t.shape[0]
        edev, _, ff = w_in.shape
        cap = 2 * tok * group_size // nexp
        src_cap = 4 * tok // nexp
        slots = edev * src_cap
        rows = NREL * src_cap
        ck = d_model // NCH
        dma = pltpu.SemaphoreType.DMA
        scratch = [
            pltpu.VMEM((NREL, NCH, tok, ck), BF16),
            pltpu.VMEM((nexp, tok), BF16),
            pltpu.VMEM((NREL, edev, tok), BF16),
            pltpu.VMEM((NREL, slots, tok), BF16),
            pltpu.VMEM((edev, NREL, src_cap, ck), BF16),
            pltpu.VMEM((edev, rows, ff), F32),
            pltpu.VMEM((rows, ff), BF16), pltpu.VMEM((rows, ff), BF16),
            pltpu.VMEM((NS1, ck, ff), BF16),
            pltpu.VMEM((NS2, ff, d_model), BF16),
            pltpu.VMEM((NREL - 1, slots, d_model), BF16),
            pltpu.VMEM((2, sum(units) * UNIT, d_model), BF16),
            pltpu.VMEM((NREL, slots, d_model), BF16),
            pltpu.VMEM((tok, d_model), F32),
            pltpu.VMEM((NREL, 8, 128), F32), pltpu.VMEM((NREL, 8, 128), F32),
            pltpu.VMEM((8, 128), F32), pltpu.VMEM((ngroups, 8, 128), F32), pltpu.VMEM((tok, 128), F32),
            dma((NS1,)), dma((NS2,)), dma((NCH,)),
            dma((NREL - 1, NCH)), dma((NREL - 1, NCH)),
            dma((NREL - 1,)), dma((NREL - 1,)),
            dma((NREL - 1,)), dma((NREL - 1,)),
            dma((ngroups - 1,)), dma((ngroups - 1,)),
            dma((1,)), dma((1,)),
            dma((2, 2)), dma((2, 2)),
        ]
        vmem = pl.BlockSpec(memory_space=pltpu.VMEM)
        hbm = pl.BlockSpec(memory_space=pl.ANY)
        return pl.pallas_call(
            functools.partial(moe_kernel, cap, units),
            out_shape=(jax.ShapeDtypeStruct((tok, d_model), BF16), jax.ShapeDtypeStruct((1,), jnp.int32)),
            in_specs=[hbm, vmem, hbm, hbm],
            out_specs=(vmem, pl.BlockSpec(memory_space=pltpu.SMEM)),
            scratch_shapes=scratch,
            compiler_params=pltpu.CompilerParams(collective_id=collective, has_side_effects=True,
                                                 vmem_limit_bytes=67000000),
        )(x_rows, logits_t, w_in, w_out)

    def local_step(x_rows, logits, w_in, w_out):
        args = (x_rows, logits.T, w_in, w_out)
        out, flag = call(PACKED, 0, *args)
        return lax.cond(flag[0] > 0, lambda: call(FULL, 1, *args)[0], lambda: out)

    return jax.shard_map(local_step, mesh=mesh, in_specs=(row_spec, row_spec, expert_spec, expert_spec),
                         out_specs=row_spec, check_vma=False)
```

```python
import functools

import jax
import jax.numpy as jnp
from jax import lax
from jax.experimental import pallas as pl
from jax.experimental.pallas import tpu as pltpu
from jax.sharding import PartitionSpec as P

BF16 = jnp.bfloat16
F32 = jnp.float32
MESH = pl.DeviceIdType.MESH
NREL = 4
NCH = 4
NS1 = 14
NS2 = 3
STEP = 4
DEFER = 4
UNIT = 16
TAIL = 2
PACKED = (0, 1, 1, 0, 1, 1, 0, 1, 0, 1, 1, 1, 0, 2, 0, 2)
SENT_ROWS = 7 / 8
FULL = (0, 2) * 8


def iota(shape, dim):
    return lax.broadcasted_iota(jnp.int32, shape, dim)


def onehot(mask):
    return mask.astype(F32).astype(BF16)


def moe_kernel(cap, units, far_rows, x_hbm, lt_ref, w1_hbm, w2_hbm, out_ref, flag_ref, xall, xp, st_own, st_far, st_all, dmat, xg, xgl, hacc, hb0, hb1,
               w1buf, w2buf, zs, pk, zr, acc, meta_own, meta_in, flag_own, flag_in, choice, w1_sem, w2_sem, xl_sem, xs_sem,
               xr_sem, ss_sem, sr_sem, ms_sem, mr_sem, fs_sem, fr_sem, ps_sem, pr_sem, zs_sem, zr_sem):
    nexp, tok = lt_ref.shape
    edev, d_model, ff = w1_hbm.shape
    src_cap = xg.shape[2]
    kmaj = edev - DEFER
    nitems = edev * NCH
    nmaj = kmaj * NCH
    slots = edev * src_cap
    ck = d_model // NCH
    rows = NREL * src_cap
    total_rows = sum(units) * UNIT
    split = total_rows - TAIL * UNIT

    me = lax.axis_index('ep')
    group = lax.axis_index('dp')
    ngroups = lax.axis_size('dp')
    mx, mc = me // 2, me % 2
    dev = [me, 2 * mx + (1 - mc), 2 * (1 - mx) + mc, 2 * (1 - mx) + (1 - mc)]

    def remote(src, dst, send, recv, r):
        return pltpu.make_async_remote_copy(src_ref=src, dst_ref=dst, send_sem=send, recv_sem=recv,
                                            device_id={'ep': dev[r]}, device_id_type=MESH)

    def w1_copy(i):
        i = jnp.int32(i)
        late = (i >= nmaj).astype(jnp.int32)
        c = (1 - late) * (i // kmaj) + late * ((i - nmaj) % NCH)
        e = (1 - late) * (i % kmaj) + late * (kmaj + (i - nmaj) // NCH)
        k = pl.multiple_of(c * ck, ck)
        s = i % NS1
        return pltpu.make_async_copy(w1_hbm.at[e, pl.ds(k, ck), :], w1buf.at[s], w1_sem.at[s])

    def w2_copy(e):
        s = e % NS2
        return pltpu.make_async_copy(w2_hbm.at[e], w2buf.at[s], w2_sem.at[s])

    def x_local(c):
        return pltpu.make_async_copy(x_hbm.at[:, pl.ds(c * ck, ck)], xall.at[0, c], xl_sem.at[c])

    def x_remote(c, slot):
        if slot == 1:
            src, dst = xall.at[0, c], xall.at[1, c]
        else:
            dst = xall.at[slot, c, pl.ds(0, far_rows), :]
            src = xp.at[c] if slot == 2 else xall.at[2, c, pl.ds(0, far_rows), :]
        return remote(src, dst, xs_sem.at[slot - 1, c], xr_sem.at[slot - 1, c], 2 if slot == 2 else 1)

    def s_remote(r):
        first = pl.multiple_of(dev[r] * edev, edev)
        src = st_own if r == 1 else st_far
        return remote(src.at[pl.ds(first, edev), :], st_all.at[r], ss_sem.at[r - 1], sr_sem.at[r - 1], r)

    def m_remote(r):
        return remote(meta_own.at[r], meta_in.at[r], ms_sem.at[r - 1], mr_sem.at[r - 1], r)

    def f_remote(k):
        peer = lax.rem(group + k, ngroups)
        return pltpu.make_async_remote_copy(src_ref=flag_own, dst_ref=flag_in.at[k], send_sem=fs_sem.at[k - 1],
                                            recv_sem=fr_sem.at[k - 1], device_id={'dp': peer}, device_id_type=MESH)

    def partner_remote(e):
        first = pl.multiple_of(e * src_cap, src_cap)
        return remote(zs.at[0, pl.ds(first, src_cap), :], zr.at[1, pl.ds(first, src_cap), :], ps_sem.at[0],
                      pr_sem.at[0], 1)

    def partner_all():
        return remote(zr.at[1], zr.at[1], ps_sem.at[0], pr_sem.at[0], 1)

    def pack_remote(r, first, size, part):
        return remote(pk.at[r - 2, pl.ds(first, size), :], zr.at[r, pl.ds(first, size), :], zs_sem.at[r - 2, part],
                      zr_sem.at[r - 2, part], r)

    def pack_part(r, part):
        span = pl.ds(0, split) if part == 0 else pl.ds(split, total_rows - split)
        ref = zr.at[r, span, :]
        return remote(ref, ref, zs_sem.at[r - 2, part], zr_sem.at[r - 2, part], r)

    barrier = pltpu.get_barrier_semaphore()
    for r in range(1, NREL):
        pl.semaphore_signal(barrier, inc=1, device_id={'ep': dev[r]}, device_id_type=MESH)
    for k in range(1, ngroups):
        pl.semaphore_signal(barrier, inc=1, device_id={'dp': lax.rem(group + k, ngroups)}, device_id_type=MESH)
    for c in range(NCH):
        x_local(c).start()

    def start_w1(i, carry):
        w1_copy(i).start()
        return carry
    lax.fori_loop(0, NS1, start_w1, 0)
    for e in range(NS2):
        w2_copy(e).start()

    for r in (2, 3):
        zs[r - 1] = jnp.zeros(zs.shape[1:], BF16)
    meta_own[...] = jnp.zeros_like(meta_own)
    if far_rows < tok:
        for r in (2, 3):
            xall[r, :, far_rows:, :] = jnp.zeros((NCH, tok - far_rows, ck), BF16)

    lt = lt_ref[...]
    m1t = jnp.max(lt, axis=0, keepdims=True)
    m2t = jnp.max(jnp.where(lt == m1t, -jnp.inf, lt), axis=0, keepdims=True)
    chosen_t = lt >= m2t
    upper = onehot(iota((tok, tok), 0) < iota((tok, tok), 1))
    before_t = jnp.dot(onehot(chosen_t), upper, preferred_element_type=F32)
    slot_t = jnp.where(chosen_t, before_t + 1.0, 0.0).astype(BF16)
    st_own[...] = slot_t
    other = iota((nexp, tok), 0) // (2 * edev) == 1 - mx
    need = jnp.max(jnp.where(jnp.logical_and(chosen_t, other), 1.0, 0.0), axis=0, keepdims=True)
    order = jnp.dot(jnp.broadcast_to(need, (UNIT, tok)).astype(BF16), upper, preferred_element_type=F32)[0:1]
    order = jnp.where(need > 0.0, order, -1.0)
    row_no = iota((tok, tok), 0)
    pack_x = onehot(jnp.logical_and(order == row_no.astype(F32), row_no < far_rows))
    over = (jnp.sum(need, axis=1, keepdims=True) > float(far_rows)).astype(F32)
    st_far[...] = lax.dot_general(slot_t, pack_x, (((1,), (1,)), ((), ())), preferred_element_type=F32).astype(BF16)
    for c in range(NCH):
        x_local(c).wait()
        xp[c] = jnp.dot(pack_x[:far_rows], xall[0, c], preferred_element_type=F32).astype(BF16)

    pl.semaphore_wait(barrier, NREL - 1 + ngroups - 1)
    for r in (2, 3, 1):
        s_remote(r).start()
    for c in range(NCH):
        x_remote(c, 2).start()
        x_remote(c, 1).start()

    logits = lt.T
    m1 = jnp.max(logits, axis=1, keepdims=True)
    is1 = logits == m1
    rest = jnp.where(is1, -jnp.inf, logits)
    m2 = jnp.max(rest, axis=1, keepdims=True)
    is2 = rest == m2
    lower = onehot(iota((tok, tok), 1) < iota((tok, tok), 0))
    before = jnp.dot(lower, onehot(jnp.logical_or(is1, is2)), preferred_element_type=F32)
    total = jnp.sum(jnp.exp(logits - m1), axis=1, keepdims=True)
    gate1 = 1.0 / total
    gate2 = jnp.exp(m2 - m1) / total

    for r in range(1, NREL):
        s_remote(r).wait_recv()
    own_first = pl.multiple_of(me * edev, edev)
    pos = [st_own[pl.ds(own_first, edev), :].astype(F32) - 1.0]
    pos += [st_all[r].astype(F32) - 1.0 for r in range(1, NREL)]
    cnt = [jnp.sum((p >= 0.0).astype(F32), axis=1, keepdims=True) for p in pos]
    ahead = []
    for r in range(NREL):
        a = jnp.zeros_like(cnt[0])
        for q in range(NREL):
            if q != r:
                a = a + cnt[q] * (dev[q] < dev[r]).astype(F32)
        ahead.append(a)

    lane_exp = iota((edev, 128), 1) - me * edev == iota((edev, 128), 0)
    exp_no = iota((edev, 1), 0)
    exp_row = exp_no.astype(F32)
    wide = iota((edev, slots), 1)
    own_slot = wide // src_cap == iota((edev, slots), 0)
    packed_row = [None, None]
    own_meta = None
    for r in range(NREL):
        if r < 2:
            base = exp_row * src_cap
            rows_kept = jnp.full((edev, 1), float(src_cap), F32)
        else:
            rows_kept = jnp.clip(cap - ahead[r], 0.0, cnt[r])
            base = jnp.zeros((edev, 1), F32)
            end = jnp.zeros((1, 1), F32)
            for e in range(edev):
                end = jnp.maximum(end, float(sum(units[:e]) * UNIT))
                base = jnp.where(exp_no == e, end, base)
                end = end + rows_kept[e:e + 1]
            over = jnp.maximum(over, (end > float(total_rows)).astype(F32))
            row = jnp.where(own_slot, base + (wide % src_cap).astype(F32), 0.0)
            row = jnp.where((wide % src_cap).astype(F32) < rows_kept, row, jnp.where(own_slot, -1.0, 0.0))
            packed_row[r - 2] = jnp.sum(row, axis=0, keepdims=True)
        base_lane = jnp.sum(jnp.where(lane_exp, base + float(r * slots), 0.0), axis=0, keepdims=True)
        kept_lane = jnp.sum(jnp.where(lane_exp, rows_kept, 0.0), axis=0, keepdims=True)
        if r == 0:
            own_meta = (base_lane, kept_lane)
        else:
            meta_own[r, 0:1, :] = base_lane
            meta_own[r, 1:2, :] = kept_lane
    for r in range(1, NREL):
        meta_own[r, 2:3, :] = jnp.broadcast_to(over, (1, 128))

    expand = onehot(iota((slots, edev), 0) // src_cap == iota((slots, edev), 1))
    slot_no = (iota((slots, tok), 0) % src_cap).astype(F32)
    for r in range(NREL):
        kept = jnp.where(pos[r] + ahead[r] < cap, pos[r], -1.0).astype(BF16)
        dmat[r] = onehot(jnp.dot(expand, kept, preferred_element_type=F32) == slot_no)
    for r in (2, 3, 1):
        m_remote(r).start()

    def relay(c):
        x_remote(c, 2).wait_recv()
        x_remote(c, 3).start()

    def gather_chunk(c):
        if c < 2:
            relay(c)
        x_remote(c, 1).wait_recv()
        for r in range(NREL):
            if r == 3:
                x_remote(c, 3).wait_recv()
            part = jnp.dot(dmat[r], xall[r, c], preferred_element_type=F32).astype(BF16)
            part = part.reshape(edev, src_cap, ck)
            xg[:, r] = part[:kmaj]
            xgl[:, c, r] = part[kmaj:]

    for c in range(NCH - 1):
        gather_chunk(c)

        def first_phase(j, carry):
            if c > 0:
                @pl.when(j == kmaj // STEP - 1)
                def _():
                    relay(c + 1)
            i0 = c * kmaj + j * STEP
            for q in range(STEP):
                w1_copy(i0 + q).wait()
            for q in range(STEP):
                e = j * STEP + q
                part = jnp.dot(xg[e].reshape(rows, ck), w1buf[(i0 + q) % NS1], preferred_element_type=F32)
                if c > 0:
                    part = hacc[e] + part
                hacc[e] = part
            for q in range(STEP):
                w1_copy(i0 + q + NS1).start()
            return carry
        lax.fori_loop(0, kmaj // STEP, first_phase, 0)

    last = (NCH - 1) * kmaj
    gather_chunk(NCH - 1)

    def place_rows():
        for r in range(1, NREL):
            m_remote(r).wait_recv()
        first_row, kept_rows = own_meta
        flag = over
        for r in range(1, NREL):
            first_row = first_row + meta_in[r, 0:1, :]
            kept_rows = kept_rows + meta_in[r, 1:2, :]
            flag = jnp.maximum(flag, meta_in[r, 2:3, 0:1])
        flag_own[...] = jnp.broadcast_to(flag, flag_own.shape)
        place = jnp.where(before < kept_rows[:, :nexp], first_row[:, :nexp] + before, -1.0)
        choice[:, 0:1] = jnp.sum(jnp.where(is1, place, 0.0), axis=1, keepdims=True)
        choice[:, 1:2] = jnp.sum(jnp.where(is2, place, 0.0), axis=1, keepdims=True)

    def w1_items(e, whole):
        return [nmaj + (e - kmaj) * NCH + c for c in range(NCH)] if whole else [last + e]

    def first_product(e, whole, hidden):
        if whole:
            h = None
            for c, i in enumerate(w1_items(e, whole)):
                part = jnp.dot(xgl[e - kmaj, c].reshape(rows, ck), w1buf[i % NS1], preferred_element_type=F32)
                h = part if h is None else h + part
        else:
            h = hacc[e] + jnp.dot(xg[e].reshape(rows, ck), w1buf[(last + e) % NS1], preferred_element_type=F32)
        hidden[...] = jax.nn.gelu(h, approximate=True).astype(BF16)

    def send_packed(e, size):
        start = sum((e > j).astype(jnp.int32) * units[j] for j in range(edev - 1) if units[j]) * UNIT
        start = pl.multiple_of(start, UNIT)
        for r in (2, 3):
            row = (iota((size, slots), 0) + start).astype(F32)
            pick = onehot(row == packed_row[r - 2])
            for c in range(NCH):
                cols = pl.ds(c * ck, ck)
                pk[r - 2, pl.ds(start, size), cols] = jnp.dot(pick, zs[r - 1, :, cols],
                                                              preferred_element_type=F32).astype(BF16)
        for r in (2, 3):
            pack_remote(r, start, size, (start >= split).astype(jnp.int32)).start()

    def expert(e, hidden, following, whole):
        items = w1_items(e + 1, whole) if following is not None else []
        for i in items:
            w1_copy(i).wait()
        w2_copy(e).wait()
        if following is not None:
            first_product(e + 1, whole, following)
        first = pl.multiple_of(e * src_cap, src_cap)
        for c in range(NCH):
            cols = pl.ds(c * ck, ck)
            z = jnp.dot(hidden[...], w2buf[e % NS2, :, cols], preferred_element_type=F32).astype(BF16)
            zr[0, pl.ds(first, src_cap), cols] = z[:src_cap]
            for r in range(1, NREL):
                zs[r - 1, pl.ds(first, src_cap), cols] = z[r * src_cap:(r + 1) * src_cap]

        @pl.when(e + NS2 < edev)
        def _():
            w2_copy(e + NS2).start()

        for i in items:
            @pl.when(i + NS1 < nitems)
            def _():
                w1_copy(i + NS1).start()

        for n in set(units) - {0}:
            @pl.when(functools.reduce(jnp.logical_or, [e == j for j in range(edev) if units[j] == n]))
            def _():
                send_packed(e, n * UNIT)
        partner_remote(e).start()

    w1_copy(last).wait()
    first_product(0, False, hb0)
    w1_copy(last + NS1).start()

    def second_phase(j, carry):
        @pl.when(j == 2)
        def _():
            place_rows()

        @pl.when(j == 4)
        def _():
            for k in range(1, ngroups):
                f_remote(k).start()
        expert(2 * j, hb0, hb1, False)
        expert(2 * j + 1, hb1, hb0, False)
        return carry
    lax.fori_loop(0, kmaj // 2 - 1, second_phase, 0)
    expert(jnp.int32(kmaj - 2), hb0, hb1, False)

    def third_phase(j, carry):
        expert(kmaj - 1 + 2 * j, hb1, hb0, True)
        expert(kmaj + 2 * j, hb0, hb1, True)
        return carry
    lax.fori_loop(0, DEFER // 2, third_phase, 0)
    expert(jnp.int32(edev - 1), hb1, None, False)

    for k in range(1, ngroups):
        f_remote(k).wait_recv()
    flag = flag_own[...]
    for k in range(1, ngroups):
        flag = jnp.maximum(flag, flag_in[k])
    flag_ref[0] = (jnp.max(flag) > 0.0).astype(jnp.int32)

    slot1, slot2 = choice[:, 0:1], choice[:, 1:2]
    far = total_rows - split
    pieces = [((0,), 0, slots), ((1,), 0, slots), ((2, 3), 0, split), ((2, 3), split, far)]
    for n, (rels, first, size) in enumerate(pieces):
        for r in rels:
            if r == 1:
                partner_all().wait_recv()
            elif r >= 2:
                pack_part(r, n - 2).wait_recv()
        slot = jnp.concatenate([(iota((1, size), 1) + (r * slots + first)).astype(F32) for r in rels], axis=1)
        pick1 = onehot(slot1 == slot)
        pick2 = onehot(slot2 == slot)
        for c in range(NCH):
            cols = pl.ds(c * ck, ck)
            zc = jnp.concatenate([zr[r, first:first + size, cols] for r in rels], axis=0)
            mix = (gate1 * jnp.dot(pick1, zc, preferred_element_type=F32)
                   + gate2 * jnp.dot(pick2, zc, preferred_element_type=F32))
            if n > 0:
                mix = acc[:, cols] + mix
            if n < len(pieces) - 1:
                acc[:, cols] = mix
            else:
                out_ref[:, cols] = (xall[0, c].astype(F32) + mix).astype(BF16)

    for k in range(1, ngroups):
        f_remote(k).wait_send()
    partner_all().wait_send()
    for r in range(1, NREL):
        s_remote(r).wait_send()
        m_remote(r).wait_send()
        for c in range(NCH):
            x_remote(c, r).wait_send()
        if r >= 2:
            for part in range(2):
                pack_part(r, part).wait_send()


def solution(mesh):
    group_size = mesh.shape['ep']
    ngroups = mesh.shape['dp']
    row_spec = P(('dp', 'ep'), None)
    expert_spec = P('ep', None, None)

    def call(units, share, collective, x_rows, logits_t, w_in, w_out):
        tok, d_model = x_rows.shape
        nexp = logits_t.shape[0]
        edev, _, ff = w_in.shape
        cap = 2 * tok * group_size // nexp
        src_cap = 4 * tok // nexp
        slots = edev * src_cap
        rows = NREL * src_cap
        ck = d_model // NCH
        far_rows = int(tok * share)
        kmaj = edev - DEFER
        dma = pltpu.SemaphoreType.DMA
        scratch = [
            pltpu.VMEM((NREL, NCH, tok, ck), BF16),
            pltpu.VMEM((NCH, far_rows, ck), BF16),
            pltpu.VMEM((nexp, tok), BF16), pltpu.VMEM((nexp, tok), BF16),
            pltpu.VMEM((NREL, edev, tok), BF16),
            pltpu.VMEM((NREL, slots, tok), BF16),
            pltpu.VMEM((kmaj, NREL, src_cap, ck), BF16),
            pltpu.VMEM((DEFER, NCH, NREL, src_cap, ck), BF16),
            pltpu.VMEM((kmaj, rows, ff), F32),
            pltpu.VMEM((rows, ff), BF16), pltpu.VMEM((rows, ff), BF16),
            pltpu.VMEM((NS1, ck, ff), BF16),
            pltpu.VMEM((NS2, ff, d_model), BF16),
            pltpu.VMEM((NREL - 1, slots, d_model), BF16),
            pltpu.VMEM((2, sum(units) * UNIT, d_model), BF16),
            pltpu.VMEM((NREL, slots, d_model), BF16),
            pltpu.VMEM((tok, d_model), F32),
            pltpu.VMEM((NREL, 8, 128), F32), pltpu.VMEM((NREL, 8, 128), F32),
            pltpu.VMEM((8, 128), F32), pltpu.VMEM((ngroups, 8, 128), F32), pltpu.VMEM((tok, 128), F32),
            dma((NS1,)), dma((NS2,)), dma((NCH,)),
            dma((NREL - 1, NCH)), dma((NREL - 1, NCH)),
            dma((NREL - 1,)), dma((NREL - 1,)),
            dma((NREL - 1,)), dma((NREL - 1,)),
            dma((ngroups - 1,)), dma((ngroups - 1,)),
            dma((1,)), dma((1,)),
            dma((2, 2)), dma((2, 2)),
        ]
        vmem = pl.BlockSpec(memory_space=pltpu.VMEM)
        hbm = pl.BlockSpec(memory_space=pl.ANY)
        return pl.pallas_call(
            functools.partial(moe_kernel, cap, units, far_rows),
            out_shape=(jax.ShapeDtypeStruct((tok, d_model), BF16), jax.ShapeDtypeStruct((1,), jnp.int32)),
            in_specs=[hbm, vmem, hbm, hbm],
            out_specs=(vmem, pl.BlockSpec(memory_space=pltpu.SMEM)),
            scratch_shapes=scratch,
            compiler_params=pltpu.CompilerParams(collective_id=collective, has_side_effects=True,
                                                 vmem_limit_bytes=67000000),
        )(x_rows, logits_t, w_in, w_out)

    def local_step(x_rows, logits, w_in, w_out):
        args = (x_rows, logits.T, w_in, w_out)
        out, flag = call(PACKED, SENT_ROWS, 0, *args)
        return lax.cond(flag[0] > 0, lambda: call(FULL, 1, 1, *args)[0], lambda: out)

    return jax.shard_map(local_step, mesh=mesh, in_specs=(row_spec, row_spec, expert_spec, expert_spec),
                         out_specs=row_spec, check_vma=False)
```

```python
import functools

import jax
import jax.numpy as jnp
from jax import lax
from jax.experimental import pallas as pl
from jax.experimental.pallas import tpu as pltpu
from jax.sharding import PartitionSpec as P

BF16 = jnp.bfloat16
F32 = jnp.float32
MESH = pl.DeviceIdType.MESH
NREL = 4
NCH = 4
NS1 = 14
NS2 = 3
STEP = 4
DEFER = 4
UNIT = 16
TAIL = 2
PACKED = (0, 1, 1, 0, 1, 1, 0, 1, 0, 1, 1, 1, 0, 2, 0, 2)
SENT_ROWS = 7 / 8
FULL = (0, 2) * 8


def iota(shape, dim):
    return lax.broadcasted_iota(jnp.int32, shape, dim)


def onehot(mask):
    return mask.astype(F32).astype(BF16)


def moe_kernel(cap, units, far_rows, x_hbm, lt_ref, w1_hbm, w2_hbm, out_ref, flag_ref, xall, xp, st_own, st_far, st_all, dmat, xg, xgl, hacc, hb0, hb1,
               w1buf, w2buf, zs, pk, zr, acc, meta_own, meta_in, flag_own, flag_in, choice, w1_sem, w2_sem, xl_sem, xs_sem,
               xr_sem, ss_sem, sr_sem, ms_sem, mr_sem, fs_sem, fr_sem, ps_sem, pr_sem, zs_sem, zr_sem):
    nexp, tok = lt_ref.shape
    edev, d_model, ff = w1_hbm.shape
    src_cap = xg.shape[2]
    kmaj = edev - DEFER
    nitems = edev * NCH
    nmaj = kmaj * NCH
    slots = edev * src_cap
    ck = d_model // NCH
    rows = NREL * src_cap
    total_rows = sum(units) * UNIT
    split = total_rows - TAIL * UNIT

    me = lax.axis_index('ep')
    group = lax.axis_index('dp')
    ngroups = lax.axis_size('dp')
    mx, mc = me // 2, me % 2
    dev = [me, 2 * mx + (1 - mc), 2 * (1 - mx) + mc, 2 * (1 - mx) + (1 - mc)]

    def remote(src, dst, send, recv, r):
        return pltpu.make_async_remote_copy(src_ref=src, dst_ref=dst, send_sem=send, recv_sem=recv,
                                            device_id={'ep': dev[r]}, device_id_type=MESH)

    def w1_copy(i):
        i = jnp.int32(i)
        late = (i >= nmaj).astype(jnp.int32)
        c = (1 - late) * (i // kmaj) + late * ((i - nmaj) % NCH)
        e = (1 - late) * (i % kmaj) + late * (kmaj + (i - nmaj) // NCH)
        k = pl.multiple_of(c * ck, ck)
        s = i % NS1
        return pltpu.make_async_copy(w1_hbm.at[e, pl.ds(k, ck), :], w1buf.at[s], w1_sem.at[s])

    def w2_copy(e):
        s = e % NS2
        return pltpu.make_async_copy(w2_hbm.at[e], w2buf.at[s], w2_sem.at[s])

    def x_local(c):
        return pltpu.make_async_copy(x_hbm.at[:, pl.ds(c * ck, ck)], xall.at[0, c], xl_sem.at[c])

    def x_remote(c, slot):
        if slot == 1:
            src, dst = xall.at[0, c], xall.at[1, c]
        else:
            dst = xall.at[slot, c, pl.ds(0, far_rows), :]
            src = xp.at[c] if slot == 2 else xall.at[2, c, pl.ds(0, far_rows), :]
        return remote(src, dst, xs_sem.at[slot - 1, c], xr_sem.at[slot - 1, c], 2 if slot == 2 else 1)

    def s_remote(r):
        first = pl.multiple_of(dev[r] * edev, edev)
        src = st_own if r == 1 else st_far
        return remote(src.at[pl.ds(first, edev), :], st_all.at[r], ss_sem.at[r - 1], sr_sem.at[r - 1], r)

    def m_remote(r):
        return remote(meta_own.at[r], meta_in.at[r], ms_sem.at[r - 1], mr_sem.at[r - 1], r)

    def f_remote(k):
        peer = lax.rem(group + k, ngroups)
        return pltpu.make_async_remote_copy(src_ref=flag_own, dst_ref=flag_in.at[k], send_sem=fs_sem.at[k - 1],
                                            recv_sem=fr_sem.at[k - 1], device_id={'dp': peer}, device_id_type=MESH)

    def partner_remote(e):
        first = pl.multiple_of(e * src_cap, src_cap)
        return remote(zs.at[0, pl.ds(first, src_cap), :], zr.at[1, pl.ds(first, src_cap), :], ps_sem.at[0],
                      pr_sem.at[0], 1)

    def partner_all():
        return remote(zr.at[1], zr.at[1], ps_sem.at[0], pr_sem.at[0], 1)

    def pack_remote(r, first, size, part):
        return remote(pk.at[r - 2, pl.ds(first, size), :], zr.at[r, pl.ds(first, size), :], zs_sem.at[r - 2, part],
                      zr_sem.at[r - 2, part], r)

    def pack_part(r, part):
        span = pl.ds(0, split) if part == 0 else pl.ds(split, total_rows - split)
        ref = zr.at[r, span, :]
        return remote(ref, ref, zs_sem.at[r - 2, part], zr_sem.at[r - 2, part], r)

    barrier = pltpu.get_barrier_semaphore()
    for r in range(1, NREL):
        pl.semaphore_signal(barrier, inc=1, device_id={'ep': dev[r]}, device_id_type=MESH)
    for k in range(1, ngroups):
        pl.semaphore_signal(barrier, inc=1, device_id={'dp': lax.rem(group + k, ngroups)}, device_id_type=MESH)
    for c in range(NCH):
        x_local(c).start()

    def start_w1(i, carry):
        w1_copy(i).start()
        return carry
    lax.fori_loop(0, NS1, start_w1, 0)
    for e in range(NS2):
        w2_copy(e).start()

    for r in (2, 3):
        zs[r - 1] = jnp.zeros(zs.shape[1:], BF16)
    meta_own[...] = jnp.zeros_like(meta_own)
    if far_rows < tok:
        for r in (2, 3):
            xall[r, :, far_rows:, :] = jnp.zeros((NCH, tok - far_rows, ck), BF16)

    lt = lt_ref[...]
    m1t = jnp.max(lt, axis=0, keepdims=True)
    m2t = jnp.max(jnp.where(lt == m1t, -jnp.inf, lt), axis=0, keepdims=True)
    chosen_t = lt >= m2t
    upper = onehot(iota((tok, tok), 0) < iota((tok, tok), 1))
    before_t = jnp.dot(onehot(chosen_t), upper, preferred_element_type=F32)
    slot_t = jnp.where(chosen_t, before_t + 1.0, 0.0).astype(BF16)
    st_own[...] = slot_t
    other = iota((nexp, tok), 0) // (2 * edev) == 1 - mx
    need = jnp.max(jnp.where(jnp.logical_and(chosen_t, other), 1.0, 0.0), axis=0, keepdims=True)
    order = jnp.dot(jnp.broadcast_to(need, (UNIT, tok)).astype(BF16), upper, preferred_element_type=F32)[0:1]
    order = jnp.where(need > 0.0, order, -1.0)
    row_no = iota((tok, tok), 0)
    pack_x = onehot(jnp.logical_and(order == row_no.astype(F32), row_no < far_rows))
    over = (jnp.sum(need, axis=1, keepdims=True) > float(far_rows)).astype(F32)
    st_far[...] = lax.dot_general(slot_t, pack_x, (((1,), (1,)), ((), ())), preferred_element_type=F32).astype(BF16)
    for c in range(NCH):
        x_local(c).wait()
        xp[c] = jnp.dot(pack_x[:far_rows], xall[0, c], preferred_element_type=F32).astype(BF16)

    pl.semaphore_wait(barrier, NREL - 1 + ngroups - 1)
    for r in (2, 3, 1):
        s_remote(r).start()
    for c in range(NCH):
        x_remote(c, 2).start()
        x_remote(c, 1).start()

    logits = lt.T
    m1 = jnp.max(logits, axis=1, keepdims=True)
    is1 = logits == m1
    rest = jnp.where(is1, -jnp.inf, logits)
    m2 = jnp.max(rest, axis=1, keepdims=True)
    is2 = rest == m2
    lower = onehot(iota((tok, tok), 1) < iota((tok, tok), 0))
    before = jnp.dot(lower, onehot(jnp.logical_or(is1, is2)), preferred_element_type=F32)
    total = jnp.sum(jnp.exp(logits - m1), axis=1, keepdims=True)
    gate1 = 1.0 / total
    gate2 = jnp.exp(m2 - m1) / total

    for r in range(1, NREL):
        s_remote(r).wait_recv()
    own_first = pl.multiple_of(me * edev, edev)
    pos = [st_own[pl.ds(own_first, edev), :].astype(F32) - 1.0]
    pos += [st_all[r].astype(F32) - 1.0 for r in range(1, NREL)]
    cnt = [jnp.sum((p >= 0.0).astype(F32), axis=1, keepdims=True) for p in pos]
    ahead = []
    for r in range(NREL):
        a = jnp.zeros_like(cnt[0])
        for q in range(NREL):
            if q != r:
                a = a + cnt[q] * (dev[q] < dev[r]).astype(F32)
        ahead.append(a)

    lane_exp = iota((edev, 128), 1) - me * edev == iota((edev, 128), 0)
    exp_no = iota((edev, 1), 0)
    exp_row = exp_no.astype(F32)
    wide = iota((edev, slots), 1)
    own_slot = wide // src_cap == iota((edev, slots), 0)
    packed_row = [None, None]
    own_meta = None
    for r in range(NREL):
        if r < 2:
            base = exp_row * src_cap
            rows_kept = jnp.full((edev, 1), float(src_cap), F32)
        else:
            rows_kept = jnp.clip(cap - ahead[r], 0.0, cnt[r])
            base = jnp.zeros((edev, 1), F32)
            end = jnp.zeros((1, 1), F32)
            for e in range(edev):
                end = jnp.maximum(end, float(sum(units[:e]) * UNIT))
                base = jnp.where(exp_no == e, end, base)
                end = end + rows_kept[e:e + 1]
            over = jnp.maximum(over, (end > float(total_rows)).astype(F32))
            row = jnp.where(own_slot, base + (wide % src_cap).astype(F32), 0.0)
            row = jnp.where((wide % src_cap).astype(F32) < rows_kept, row, jnp.where(own_slot, -1.0, 0.0))
            packed_row[r - 2] = jnp.sum(row, axis=0, keepdims=True)
        base_lane = jnp.sum(jnp.where(lane_exp, base + float(r * slots), 0.0), axis=0, keepdims=True)
        kept_lane = jnp.sum(jnp.where(lane_exp, rows_kept, 0.0), axis=0, keepdims=True)
        if r == 0:
            own_meta = (base_lane, kept_lane)
        else:
            meta_own[r, 0:1, :] = base_lane
            meta_own[r, 1:2, :] = kept_lane
    for r in range(1, NREL):
        meta_own[r, 2:3, :] = jnp.broadcast_to(over, (1, 128))

    expand = onehot(iota((slots, edev), 0) // src_cap == iota((slots, edev), 1))
    slot_no = (iota((slots, tok), 0) % src_cap).astype(F32)
    for r in range(NREL):
        kept = jnp.where(pos[r] + ahead[r] < cap, pos[r], -1.0).astype(BF16)
        dmat[r] = onehot(jnp.dot(expand, kept, preferred_element_type=F32) == slot_no)
    for r in (2, 3, 1):
        m_remote(r).start()

    def relay(c):
        x_remote(c, 2).wait_recv()
        x_remote(c, 3).start()

    def gather_chunk(c):
        if c < 2:
            relay(c)
        x_remote(c, 1).wait_recv()
        for r in range(NREL):
            if r == 3:
                x_remote(c, 3).wait_recv()
            part = jnp.dot(dmat[r], xall[r, c], preferred_element_type=F32).astype(BF16)
            part = part.reshape(edev, src_cap, ck)
            xg[:, r] = part[:kmaj]
            xgl[:, c, r] = part[kmaj:]

    for c in range(NCH - 1):
        gather_chunk(c)

        def first_phase(j, carry):
            if c > 0:
                @pl.when(j == kmaj // STEP - 1)
                def _():
                    relay(c + 1)
            i0 = c * kmaj + j * STEP
            for q in range(STEP):
                w1_copy(i0 + q).wait()
            for q in range(STEP):
                e = j * STEP + q
                part = jnp.dot(xg[e].reshape(rows, ck), w1buf[(i0 + q) % NS1], preferred_element_type=F32)
                if c > 0:
                    part = hacc[e] + part
                hacc[e] = part
            for q in range(STEP):
                w1_copy(i0 + q + NS1).start()
            return carry
        lax.fori_loop(0, kmaj // STEP, first_phase, 0)

    last = (NCH - 1) * kmaj
    gather_chunk(NCH - 1)

    def place_rows():
        for r in range(1, NREL):
            m_remote(r).wait_recv()
        first_row, kept_rows = own_meta
        flag = over
        for r in range(1, NREL):
            first_row = first_row + meta_in[r, 0:1, :]
            kept_rows = kept_rows + meta_in[r, 1:2, :]
            flag = jnp.maximum(flag, meta_in[r, 2:3, 0:1])
        flag_own[...] = jnp.broadcast_to(flag, flag_own.shape)
        place = jnp.where(before < kept_rows[:, :nexp], first_row[:, :nexp] + before, -1.0)
        choice[:, 0:1] = jnp.sum(jnp.where(is1, place, 0.0), axis=1, keepdims=True)
        choice[:, 1:2] = jnp.sum(jnp.where(is2, place, 0.0), axis=1, keepdims=True)

    def w1_items(e, whole):
        return [nmaj + (e - kmaj) * NCH + c for c in range(NCH)] if whole else [last + e]

    def first_product(e, whole, hidden):
        if whole:
            h = None
            for c, i in enumerate(w1_items(e, whole)):
                part = jnp.dot(xgl[e - kmaj, c].reshape(rows, ck), w1buf[i % NS1], preferred_element_type=F32)
                h = part if h is None else h + part
        else:
            h = hacc[e] + jnp.dot(xg[e].reshape(rows, ck), w1buf[(last + e) % NS1], preferred_element_type=F32)
        hidden[...] = jax.nn.gelu(h, approximate=True).astype(BF16)

    def send_packed(e, size):
        start = sum((e > j).astype(jnp.int32) * units[j] for j in range(edev - 1) if units[j]) * UNIT
        start = pl.multiple_of(start, UNIT)
        for r in (2, 3):
            row = (iota((size, slots), 0) + start).astype(F32)
            pick = onehot(row == packed_row[r - 2])
            for c in range(NCH):
                cols = pl.ds(c * ck, ck)
                pk[r - 2, pl.ds(start, size), cols] = jnp.dot(pick, zs[r - 1, :, cols],
                                                              preferred_element_type=F32).astype(BF16)
        for r in (2, 3):
            pack_remote(r, start, size, (start >= split).astype(jnp.int32)).start()

    def expert(e, hidden, following, whole):
        items = w1_items(e + 1, whole) if following is not None else []
        for i in items:
            w1_copy(i).wait()
        w2_copy(e).wait()
        if following is not None:
            first_product(e + 1, whole, following)
        first = pl.multiple_of(e * src_cap, src_cap)
        for c in range(NCH):
            cols = pl.ds(c * ck, ck)
            z = jnp.dot(hidden[...], w2buf[e % NS2, :, cols], preferred_element_type=F32).astype(BF16)
            zr[0, pl.ds(first, src_cap), cols] = z[:src_cap]
            for r in range(1, NREL):
                zs[r - 1, pl.ds(first, src_cap), cols] = z[r * src_cap:(r + 1) * src_cap]

        @pl.when(e + NS2 < edev)
        def _():
            w2_copy(e + NS2).start()

        for i in items:
            @pl.when(i + NS1 < nitems)
            def _():
                w1_copy(i + NS1).start()

        for n in set(units) - {0}:
            @pl.when(functools.reduce(jnp.logical_or, [e == j for j in range(edev) if units[j] == n]))
            def _():
                send_packed(e, n * UNIT)
        partner_remote(e).start()

    w1_copy(last).wait()
    first_product(0, False, hb0)
    w1_copy(last + NS1).start()

    def second_phase(j, carry):
        @pl.when(j == 2)
        def _():
            place_rows()

        @pl.when(j == 4)
        def _():
            for k in range(1, ngroups):
                f_remote(k).start()
        expert(2 * j, hb0, hb1, False)
        expert(2 * j + 1, hb1, hb0, False)
        return carry
    lax.fori_loop(0, kmaj // 2 - 1, second_phase, 0)
    expert(jnp.int32(kmaj - 2), hb0, hb1, False)

    def third_phase(j, carry):
        expert(kmaj - 1 + 2 * j, hb1, hb0, True)
        expert(kmaj + 2 * j, hb0, hb1, True)
        return carry
    lax.fori_loop(0, DEFER // 2, third_phase, 0)
    expert(jnp.int32(edev - 1), hb1, None, False)

    for k in range(1, ngroups):
        f_remote(k).wait_recv()
    flag = flag_own[...]
    for k in range(1, ngroups):
        flag = jnp.maximum(flag, flag_in[k])
    flag_ref[0] = (jnp.max(flag) > 0.0).astype(jnp.int32)

    slot1, slot2 = choice[:, 0:1], choice[:, 1:2]
    far = total_rows - split
    pieces = [((0,), 0, slots), ((1,), 0, slots), ((2, 3), 0, split), ((2, 3), split, far)]
    for n, (rels, first, size) in enumerate(pieces):
        for r in rels:
            if r == 1:
                partner_all().wait_recv()
            elif r >= 2:
                pack_part(r, n - 2).wait_recv()
        slot = jnp.concatenate([(iota((1, size), 1) + (r * slots + first)).astype(F32) for r in rels], axis=1)
        pick1 = onehot(slot1 == slot)
        pick2 = onehot(slot2 == slot)
        for c in range(NCH):
            cols = pl.ds(c * ck, ck)
            zc = jnp.concatenate([zr[r, first:first + size, cols] for r in rels], axis=0)
            mix = (gate1 * jnp.dot(pick1, zc, preferred_element_type=F32)
                   + gate2 * jnp.dot(pick2, zc, preferred_element_type=F32))
            if n > 0:
                mix = acc[:, cols] + mix
            if n < len(pieces) - 1:
                acc[:, cols] = mix
            else:
                out_ref[:, cols] = (xall[0, c].astype(F32) + mix).astype(BF16)

    for k in range(1, ngroups):
        f_remote(k).wait_send()
    partner_all().wait_send()
    for r in range(1, NREL):
        s_remote(r).wait_send()
        m_remote(r).wait_send()
        for c in range(NCH):
            x_remote(c, r).wait_send()
        if r >= 2:
            for part in range(2):
                pack_part(r, part).wait_send()


def solution(mesh):
    group_size = mesh.shape['ep']
    ngroups = mesh.shape['dp']
    row_spec = P(('dp', 'ep'), None)
    expert_spec = P('ep', None, None)

    def call(units, share, collective, x_rows, logits_t, w_in, w_out):
        tok, d_model = x_rows.shape
        nexp = logits_t.shape[0]
        edev, _, ff = w_in.shape
        cap = 2 * tok * group_size // nexp
        src_cap = 4 * tok // nexp
        slots = edev * src_cap
        rows = NREL * src_cap
        ck = d_model // NCH
        far_rows = int(tok * share)
        kmaj = edev - DEFER
        dma = pltpu.SemaphoreType.DMA
        scratch = [
            pltpu.VMEM((NREL, NCH, tok, ck), BF16),
            pltpu.VMEM((NCH, far_rows, ck), BF16),
            pltpu.VMEM((nexp, tok), BF16), pltpu.VMEM((nexp, tok), BF16),
            pltpu.VMEM((NREL, edev, tok), BF16),
            pltpu.VMEM((NREL, slots, tok), BF16),
            pltpu.VMEM((kmaj, NREL, src_cap, ck), BF16),
            pltpu.VMEM((DEFER, NCH, NREL, src_cap, ck), BF16),
            pltpu.VMEM((kmaj, rows, ff), F32),
            pltpu.VMEM((rows, ff), BF16), pltpu.VMEM((rows, ff), BF16),
            pltpu.VMEM((NS1, ck, ff), BF16),
            pltpu.VMEM((NS2, ff, d_model), BF16),
            pltpu.VMEM((NREL - 1, slots, d_model), BF16),
            pltpu.VMEM((2, sum(units) * UNIT, d_model), BF16),
            pltpu.VMEM((NREL, slots, d_model), BF16),
            pltpu.VMEM((tok, d_model), F32),
            pltpu.VMEM((NREL, 8, 128), F32), pltpu.VMEM((NREL, 8, 128), F32),
            pltpu.VMEM((8, 128), F32), pltpu.VMEM((ngroups, 8, 128), F32), pltpu.VMEM((tok, 128), F32),
            dma((NS1,)), dma((NS2,)), dma((NCH,)),
            dma((NREL - 1, NCH)), dma((NREL - 1, NCH)),
            dma((NREL - 1,)), dma((NREL - 1,)),
            dma((NREL - 1,)), dma((NREL - 1,)),
            dma((ngroups - 1,)), dma((ngroups - 1,)),
            dma((1,)), dma((1,)),
            dma((2, 2)), dma((2, 2)),
        ]
        vmem = pl.BlockSpec(memory_space=pltpu.VMEM)
        hbm = pl.BlockSpec(memory_space=pl.ANY)
        return pl.pallas_call(
            functools.partial(moe_kernel, cap, units, far_rows),
            out_shape=(pltpu.VMEM((tok, d_model), BF16), pltpu.SMEM((1,), jnp.int32)),
            in_specs=[hbm, vmem, hbm, hbm],
            out_specs=(vmem, pl.BlockSpec(memory_space=pltpu.SMEM)),
            scratch_shapes=scratch,
            compiler_params=pltpu.CompilerParams(collective_id=collective, has_side_effects=True,
                                                 vmem_limit_bytes=65900000),
        )(x_rows, logits_t, w_in, w_out)

    def local_step(x_rows, logits, w_in, w_out):
        args = (x_rows, logits.T, w_in, w_out)
        out, flag = call(PACKED, SENT_ROWS, 0, *args)
        return lax.cond(flag[0] > 0, lambda: call(FULL, 1, 1, *args)[0], lambda: out)

    return jax.shard_map(local_step, mesh=mesh, in_specs=(row_spec, row_spec, expert_spec, expert_spec),
                         out_specs=row_spec, check_vma=False)
```

```python
import functools

import jax
import jax.numpy as jnp
from jax import lax
from jax.experimental import pallas as pl
from jax.experimental.pallas import tpu as pltpu
from jax.sharding import PartitionSpec as P

BF16 = jnp.bfloat16
F32 = jnp.float32
MESH = pl.DeviceIdType.MESH
NREL = 4
NCH = 4
NS1 = 14
NS2 = 3
STEP = 4
DEFER = 4
UNIT = 16
TAIL = 2
PACKED = (0, 1, 1, 0, 1, 1, 0, 1, 0, 1, 1, 1, 1, 1, 0, 2)
SENT_ROWS = 7 / 8
FULL = (0, 2) * 8


def iota(shape, dim):
    return lax.broadcasted_iota(jnp.int32, shape, dim)


def onehot(mask):
    return mask.astype(F32).astype(BF16)


def moe_kernel(cap, units, far_rows, x_hbm, lt_ref, w1_hbm, w2_hbm, out_ref, flag_ref, xall, xp, st_own, st_far, st_all, dmat, xg, xgl, hacc, hb0, hb1,
               w1buf, w2buf, zs, pk, zr, acc, meta_own, meta_in, flag_own, flag_in, choice, w1_sem, w2_sem, xl_sem, xs_sem,
               xr_sem, ss_sem, sr_sem, ms_sem, mr_sem, fs_sem, fr_sem, ps_sem, pr_sem, zs_sem, zr_sem):
    nexp, tok = lt_ref.shape
    edev, d_model, ff = w1_hbm.shape
    src_cap = xg.shape[2]
    kmaj = edev - DEFER
    nitems = edev * NCH
    nmaj = kmaj * NCH
    slots = edev * src_cap
    ck = d_model // NCH
    rows = NREL * src_cap
    total_rows = sum(units) * UNIT
    split = total_rows - TAIL * UNIT

    me = lax.axis_index('ep')
    group = lax.axis_index('dp')
    ngroups = lax.axis_size('dp')
    mx, mc = me // 2, me % 2
    dev = [me, 2 * mx + (1 - mc), 2 * (1 - mx) + mc, 2 * (1 - mx) + (1 - mc)]

    def remote(src, dst, send, recv, r):
        return pltpu.make_async_remote_copy(src_ref=src, dst_ref=dst, send_sem=send, recv_sem=recv,
                                            device_id={'ep': dev[r]}, device_id_type=MESH)

    def w1_copy(i):
        i = jnp.int32(i)
        late = (i >= nmaj).astype(jnp.int32)
        c = (1 - late) * (i // kmaj) + late * ((i - nmaj) % NCH)
        e = (1 - late) * (i % kmaj) + late * (kmaj + (i - nmaj) // NCH)
        k = pl.multiple_of(c * ck, ck)
        s = i % NS1
        return pltpu.make_async_copy(w1_hbm.at[e, pl.ds(k, ck), :], w1buf.at[s], w1_sem.at[s])

    def w2_copy(e):
        s = e % NS2
        return pltpu.make_async_copy(w2_hbm.at[e], w2buf.at[s], w2_sem.at[s])

    def x_local(c):
        return pltpu.make_async_copy(x_hbm.at[:, pl.ds(c * ck, ck)], xall.at[0, c], xl_sem.at[c])

    def x_remote(c, slot):
        if slot == 1:
            src, dst = xall.at[0, c], xall.at[1, c]
        else:
            dst = xall.at[slot, c, pl.ds(0, far_rows), :]
            src = xp.at[c] if slot == 2 else xall.at[2, c, pl.ds(0, far_rows), :]
        return remote(src, dst, xs_sem.at[slot - 1, c], xr_sem.at[slot - 1, c], 2 if slot == 2 else 1)

    def s_remote(r):
        first = pl.multiple_of(dev[r] * edev, edev)
        src = st_own if r == 1 else st_far
        return remote(src.at[pl.ds(first, edev), :], st_all.at[r], ss_sem.at[r - 1], sr_sem.at[r - 1], r)

    def m_remote(r):
        return remote(meta_own.at[r], meta_in.at[r], ms_sem.at[r - 1], mr_sem.at[r - 1], r)

    def f_remote(k):
        peer = lax.rem(group + k, ngroups)
        return pltpu.make_async_remote_copy(src_ref=flag_own, dst_ref=flag_in.at[k], send_sem=fs_sem.at[k - 1],
                                            recv_sem=fr_sem.at[k - 1], device_id={'dp': peer}, device_id_type=MESH)

    def partner_remote(e):
        first = pl.multiple_of(e * src_cap, src_cap)
        return remote(zs.at[0, pl.ds(first, src_cap), :], zr.at[1, pl.ds(first, src_cap), :], ps_sem.at[0],
                      pr_sem.at[0], 1)

    def partner_all():
        return remote(zr.at[1], zr.at[1], ps_sem.at[0], pr_sem.at[0], 1)

    def pack_remote(r, first, size, part):
        return remote(pk.at[r - 2, pl.ds(first, size), :], zr.at[r, pl.ds(first, size), :], zs_sem.at[r - 2, part],
                      zr_sem.at[r - 2, part], r)

    def pack_part(r, part):
        span = pl.ds(0, split) if part == 0 else pl.ds(split, total_rows - split)
        ref = zr.at[r, span, :]
        return remote(ref, ref, zs_sem.at[r - 2, part], zr_sem.at[r - 2, part], r)

    barrier = pltpu.get_barrier_semaphore()
    for r in range(1, NREL):
        pl.semaphore_signal(barrier, inc=1, device_id={'ep': dev[r]}, device_id_type=MESH)
    for k in range(1, ngroups):
        pl.semaphore_signal(barrier, inc=1, device_id={'dp': lax.rem(group + k, ngroups)}, device_id_type=MESH)
    for c in range(NCH):
        x_local(c).start()

    def start_w1(i, carry):
        w1_copy(i).start()
        return carry
    lax.fori_loop(0, NS1, start_w1, 0)
    for e in range(NS2):
        w2_copy(e).start()

    for r in (2, 3):
        zs[r - 1] = jnp.zeros(zs.shape[1:], BF16)
    meta_own[...] = jnp.zeros_like(meta_own)
    if far_rows < tok:
        for r in (2, 3):
            xall[r, :, far_rows:, :] = jnp.zeros((NCH, tok - far_rows, ck), BF16)

    lt = lt_ref[...]
    m1t = jnp.max(lt, axis=0, keepdims=True)
    m2t = jnp.max(jnp.where(lt == m1t, -jnp.inf, lt), axis=0, keepdims=True)
    chosen_t = lt >= m2t
    upper = onehot(iota((tok, tok), 0) < iota((tok, tok), 1))
    before_t = jnp.dot(onehot(chosen_t), upper, preferred_element_type=F32)
    slot_t = jnp.where(chosen_t, before_t + 1.0, 0.0).astype(BF16)
    st_own[...] = slot_t
    other = iota((nexp, tok), 0) // (2 * edev) == 1 - mx
    need = jnp.max(jnp.where(jnp.logical_and(chosen_t, other), 1.0, 0.0), axis=0, keepdims=True)
    order = jnp.dot(jnp.broadcast_to(need, (UNIT, tok)).astype(BF16), upper, preferred_element_type=F32)[0:1]
    order = jnp.where(need > 0.0, order, -1.0)
    row_no = iota((tok, tok), 0)
    pack_x = onehot(jnp.logical_and(order == row_no.astype(F32), row_no < far_rows))
    over = (jnp.sum(need, axis=1, keepdims=True) > float(far_rows)).astype(F32)
    st_far[...] = lax.dot_general(slot_t, pack_x, (((1,), (1,)), ((), ())), preferred_element_type=F32).astype(BF16)
    for c in range(NCH):
        x_local(c).wait()
        xp[c] = jnp.dot(pack_x[:far_rows], xall[0, c], preferred_element_type=F32).astype(BF16)

    pl.semaphore_wait(barrier, NREL - 1 + ngroups - 1)
    for r in (2, 3, 1):
        s_remote(r).start()
    for c in range(NCH):
        x_remote(c, 2).start()
        x_remote(c, 1).start()

    logits = lt.T
    m1 = jnp.max(logits, axis=1, keepdims=True)
    is1 = logits == m1
    rest = jnp.where(is1, -jnp.inf, logits)
    m2 = jnp.max(rest, axis=1, keepdims=True)
    is2 = rest == m2
    lower = onehot(iota((tok, tok), 1) < iota((tok, tok), 0))
    before = jnp.dot(lower, onehot(jnp.logical_or(is1, is2)), preferred_element_type=F32)
    total = jnp.sum(jnp.exp(logits - m1), axis=1, keepdims=True)
    gate1 = 1.0 / total
    gate2 = jnp.exp(m2 - m1) / total

    for r in range(1, NREL):
        s_remote(r).wait_recv()
    own_first = pl.multiple_of(me * edev, edev)
    pos = [st_own[pl.ds(own_first, edev), :].astype(F32) - 1.0]
    pos += [st_all[r].astype(F32) - 1.0 for r in range(1, NREL)]
    cnt = [jnp.sum((p >= 0.0).astype(F32), axis=1, keepdims=True) for p in pos]
    ahead = []
    for r in range(NREL):
        a = jnp.zeros_like(cnt[0])
        for q in range(NREL):
            if q != r:
                a = a + cnt[q] * (dev[q] < dev[r]).astype(F32)
        ahead.append(a)

    lane_exp = iota((edev, 128), 1) - me * edev == iota((edev, 128), 0)
    exp_no = iota((edev, 1), 0)
    exp_row = exp_no.astype(F32)
    wide = iota((edev, slots), 1)
    own_slot = wide // src_cap == iota((edev, slots), 0)
    packed_row = [None, None]
    own_meta = None
    for r in range(NREL):
        if r < 2:
            base = exp_row * src_cap
            rows_kept = jnp.full((edev, 1), float(src_cap), F32)
        else:
            rows_kept = jnp.clip(cap - ahead[r], 0.0, cnt[r])
            base = jnp.zeros((edev, 1), F32)
            end = jnp.zeros((1, 1), F32)
            for e in range(edev):
                end = jnp.maximum(end, float(sum(units[:e]) * UNIT))
                base = jnp.where(exp_no == e, end, base)
                end = end + rows_kept[e:e + 1]
            over = jnp.maximum(over, (end > float(total_rows)).astype(F32))
            row = jnp.where(own_slot, base + (wide % src_cap).astype(F32), 0.0)
            row = jnp.where((wide % src_cap).astype(F32) < rows_kept, row, jnp.where(own_slot, -1.0, 0.0))
            packed_row[r - 2] = jnp.sum(row, axis=0, keepdims=True)
        base_lane = jnp.sum(jnp.where(lane_exp, base + float(r * slots), 0.0), axis=0, keepdims=True)
        kept_lane = jnp.sum(jnp.where(lane_exp, rows_kept, 0.0), axis=0, keepdims=True)
        if r == 0:
            own_meta = (base_lane, kept_lane)
        else:
            meta_own[r, 0:1, :] = base_lane
            meta_own[r, 1:2, :] = kept_lane
    for r in range(1, NREL):
        meta_own[r, 2:3, :] = jnp.broadcast_to(over, (1, 128))

    expand = onehot(iota((slots, edev), 0) // src_cap == iota((slots, edev), 1))
    slot_no = (iota((slots, tok), 0) % src_cap).astype(F32)
    for r in range(NREL):
        kept = jnp.where(pos[r] + ahead[r] < cap, pos[r], -1.0).astype(BF16)
        dmat[r] = onehot(jnp.dot(expand, kept, preferred_element_type=F32) == slot_no)
    for r in (2, 3, 1):
        m_remote(r).start()

    def relay(c):
        x_remote(c, 2).wait_recv()
        x_remote(c, 3).start()

    def gather_chunk(c):
        if c < 2:
            relay(c)
        x_remote(c, 1).wait_recv()
        for r in range(NREL):
            if r == 3:
                x_remote(c, 3).wait_recv()
            part = jnp.dot(dmat[r], xall[r, c], preferred_element_type=F32).astype(BF16)
            part = part.reshape(edev, src_cap, ck)
            xg[:, r] = part[:kmaj]
            xgl[:, c, r] = part[kmaj:]

    for c in range(NCH - 1):
        gather_chunk(c)

        def first_phase(j, carry):
            if c > 0:
                @pl.when(j == kmaj // STEP - 1)
                def _():
                    relay(c + 1)
            i0 = c * kmaj + j * STEP
            for q in range(STEP):
                w1_copy(i0 + q).wait()
            for q in range(STEP):
                e = j * STEP + q
                part = jnp.dot(xg[e].reshape(rows, ck), w1buf[(i0 + q) % NS1], preferred_element_type=F32)
                if c > 0:
                    part = hacc[e] + part
                hacc[e] = part
            for q in range(STEP):
                w1_copy(i0 + q + NS1).start()
            return carry
        lax.fori_loop(0, kmaj // STEP, first_phase, 0)

    last = (NCH - 1) * kmaj
    gather_chunk(NCH - 1)

    def place_rows():
        for r in range(1, NREL):
            m_remote(r).wait_recv()
        first_row, kept_rows = own_meta
        flag = over
        for r in range(1, NREL):
            first_row = first_row + meta_in[r, 0:1, :]
            kept_rows = kept_rows + meta_in[r, 1:2, :]
            flag = jnp.maximum(flag, meta_in[r, 2:3, 0:1])
        flag_own[...] = jnp.broadcast_to(flag, flag_own.shape)
        place = jnp.where(before < kept_rows[:, :nexp], first_row[:, :nexp] + before, -1.0)
        choice[:, 0:1] = jnp.sum(jnp.where(is1, place, 0.0), axis=1, keepdims=True)
        choice[:, 1:2] = jnp.sum(jnp.where(is2, place, 0.0), axis=1, keepdims=True)

    def w1_items(e, whole):
        return [nmaj + (e - kmaj) * NCH + c for c in range(NCH)] if whole else [last + e]

    def first_product(e, whole, hidden):
        if whole:
            h = None
            for c, i in enumerate(w1_items(e, whole)):
                part = jnp.dot(xgl[e - kmaj, c].reshape(rows, ck), w1buf[i % NS1], preferred_element_type=F32)
                h = part if h is None else h + part
        else:
            h = hacc[e] + jnp.dot(xg[e].reshape(rows, ck), w1buf[(last + e) % NS1], preferred_element_type=F32)
        hidden[...] = jax.nn.gelu(h, approximate=True).astype(BF16)

    def send_packed(e, size):
        start = sum((e > j).astype(jnp.int32) * units[j] for j in range(edev - 1) if units[j]) * UNIT
        start = pl.multiple_of(start, UNIT)
        for r in (2, 3):
            row = (iota((size, slots), 0) + start).astype(F32)
            pick = onehot(row == packed_row[r - 2])
            for c in range(NCH):
                cols = pl.ds(c * ck, ck)
                pk[r - 2, pl.ds(start, size), cols] = jnp.dot(pick, zs[r - 1, :, cols],
                                                              preferred_element_type=F32).astype(BF16)
        for r in (2, 3):
            pack_remote(r, start, size, (start >= split).astype(jnp.int32)).start()

    def expert(e, hidden, following, whole):
        items = w1_items(e + 1, whole) if following is not None else []
        for i in items:
            w1_copy(i).wait()
        w2_copy(e).wait()
        if following is not None:
            first_product(e + 1, whole, following)
        first = pl.multiple_of(e * src_cap, src_cap)
        for c in range(NCH):
            cols = pl.ds(c * ck, ck)
            z = jnp.dot(hidden[...], w2buf[e % NS2, :, cols], preferred_element_type=F32).astype(BF16)
            zr[0, pl.ds(first, src_cap), cols] = z[:src_cap]
            for r in range(1, NREL):
                zs[r - 1, pl.ds(first, src_cap), cols] = z[r * src_cap:(r + 1) * src_cap]

        @pl.when(e + NS2 < edev)
        def _():
            w2_copy(e + NS2).start()

        for i in items:
            @pl.when(i + NS1 < nitems)
            def _():
                w1_copy(i + NS1).start()

        for n in set(units) - {0}:
            @pl.when(functools.reduce(jnp.logical_or, [e == j for j in range(edev) if units[j] == n]))
            def _():
                send_packed(e, n * UNIT)
        partner_remote(e).start()

    w1_copy(last).wait()
    first_product(0, False, hb0)
    w1_copy(last + NS1).start()

    def second_phase(j, carry):
        @pl.when(j == 2)
        def _():
            place_rows()

        @pl.when(j == 4)
        def _():
            for k in range(1, ngroups):
                f_remote(k).start()
        expert(2 * j, hb0, hb1, False)
        expert(2 * j + 1, hb1, hb0, False)
        return carry
    lax.fori_loop(0, kmaj // 2 - 1, second_phase, 0)
    expert(jnp.int32(kmaj - 2), hb0, hb1, False)

    def third_phase(j, carry):
        expert(kmaj - 1 + 2 * j, hb1, hb0, True)
        expert(kmaj + 2 * j, hb0, hb1, True)
        return carry
    lax.fori_loop(0, DEFER // 2, third_phase, 0)
    expert(jnp.int32(edev - 1), hb1, None, False)

    for k in range(1, ngroups):
        f_remote(k).wait_recv()
    flag = flag_own[...]
    for k in range(1, ngroups):
        flag = jnp.maximum(flag, flag_in[k])
    flag_ref[0] = (jnp.max(flag) > 0.0).astype(jnp.int32)

    slot1, slot2 = choice[:, 0:1], choice[:, 1:2]
    far = total_rows - split
    pieces = [((0,), 0, slots), ((1,), 0, slots), ((2, 3), 0, split), ((2, 3), split, far)]
    for n, (rels, first, size) in enumerate(pieces):
        for r in rels:
            if r == 1:
                partner_all().wait_recv()
            elif r >= 2:
                pack_part(r, n - 2).wait_recv()
        slot = jnp.concatenate([(iota((1, size), 1) + (r * slots + first)).astype(F32) for r in rels], axis=1)
        pick1 = onehot(slot1 == slot)
        pick2 = onehot(slot2 == slot)
        for c in range(NCH):
            cols = pl.ds(c * ck, ck)
            zc = jnp.concatenate([zr[r, first:first + size, cols] for r in rels], axis=0)
            mix = (gate1 * jnp.dot(pick1, zc, preferred_element_type=F32)
                   + gate2 * jnp.dot(pick2, zc, preferred_element_type=F32))
            if n > 0:
                mix = acc[:, cols] + mix
            if n < len(pieces) - 1:
                acc[:, cols] = mix
            else:
                out_ref[:, cols] = (xall[0, c].astype(F32) + mix).astype(BF16)

    for k in range(1, ngroups):
        f_remote(k).wait_send()
    partner_all().wait_send()
    for r in range(1, NREL):
        s_remote(r).wait_send()
        m_remote(r).wait_send()
        for c in range(NCH):
            x_remote(c, r).wait_send()
        if r >= 2:
            for part in range(2):
                pack_part(r, part).wait_send()


def solution(mesh):
    group_size = mesh.shape['ep']
    ngroups = mesh.shape['dp']
    row_spec = P(('dp', 'ep'), None)
    expert_spec = P('ep', None, None)

    def call(units, share, collective, x_rows, logits_t, w_in, w_out):
        tok, d_model = x_rows.shape
        nexp = logits_t.shape[0]
        edev, _, ff = w_in.shape
        cap = 2 * tok * group_size // nexp
        src_cap = 4 * tok // nexp
        slots = edev * src_cap
        rows = NREL * src_cap
        ck = d_model // NCH
        far_rows = int(tok * share)
        kmaj = edev - DEFER
        dma = pltpu.SemaphoreType.DMA
        scratch = [
            pltpu.VMEM((NREL, NCH, tok, ck), BF16),
            pltpu.VMEM((NCH, far_rows, ck), BF16),
            pltpu.VMEM((nexp, tok), BF16), pltpu.VMEM((nexp, tok), BF16),
            pltpu.VMEM((NREL, edev, tok), BF16),
            pltpu.VMEM((NREL, slots, tok), BF16),
            pltpu.VMEM((kmaj, NREL, src_cap, ck), BF16),
            pltpu.VMEM((DEFER, NCH, NREL, src_cap, ck), BF16),
            pltpu.VMEM((kmaj, rows, ff), F32),
            pltpu.VMEM((rows, ff), BF16), pltpu.VMEM((rows, ff), BF16),
            pltpu.VMEM((NS1, ck, ff), BF16),
            pltpu.VMEM((NS2, ff, d_model), BF16),
            pltpu.VMEM((NREL - 1, slots, d_model), BF16),
            pltpu.VMEM((2, sum(units) * UNIT, d_model), BF16),
            pltpu.VMEM((NREL, slots, d_model), BF16),
            pltpu.VMEM((tok, d_model), F32),
            pltpu.VMEM((NREL, 8, 128), F32), pltpu.VMEM((NREL, 8, 128), F32),
            pltpu.VMEM((8, 128), F32), pltpu.VMEM((ngroups, 8, 128), F32), pltpu.VMEM((tok, 128), F32),
            dma((NS1,)), dma((NS2,)), dma((NCH,)),
            dma((NREL - 1, NCH)), dma((NREL - 1, NCH)),
            dma((NREL - 1,)), dma((NREL - 1,)),
            dma((NREL - 1,)), dma((NREL - 1,)),
            dma((ngroups - 1,)), dma((ngroups - 1,)),
            dma((1,)), dma((1,)),
            dma((2, 2)), dma((2, 2)),
        ]
        vmem = pl.BlockSpec(memory_space=pltpu.VMEM)
        hbm = pl.BlockSpec(memory_space=pl.ANY)
        return pl.pallas_call(
            functools.partial(moe_kernel, cap, units, far_rows),
            out_shape=(pltpu.VMEM((tok, d_model), BF16), pltpu.SMEM((1,), jnp.int32)),
            in_specs=[hbm, vmem, hbm, hbm],
            out_specs=(vmem, pl.BlockSpec(memory_space=pltpu.SMEM)),
            scratch_shapes=scratch,
            compiler_params=pltpu.CompilerParams(collective_id=collective, has_side_effects=True,
                                                 vmem_limit_bytes=65900000),
        )(x_rows, logits_t, w_in, w_out)

    def local_step(x_rows, logits, w_in, w_out):
        args = (x_rows, logits.T, w_in, w_out)
        out, flag = call(PACKED, SENT_ROWS, 0, *args)
        return lax.cond(flag[0] > 0, lambda: call(FULL, 1, 1, *args)[0], lambda: out)

    return jax.shard_map(local_step, mesh=mesh, in_specs=(row_spec, row_spec, expert_spec, expert_spec),
                         out_specs=row_spec, check_vma=False)
```
